32 devices in a mesh: gx: 4 (over z), gy: 4 (over y, core), gz: 2 (over x).
Axes of the slice: x: 2, y: 2, z: 4, core: 2. Of those that a mesh axis runs over, the one named last changes fastest.
Arguments:
- point_data: float32 [1, 6, 16384], P(None, None, ('gx', 'gy', 'gz')), may hold values from -1 to 1
- neighbours: int32 [1, 64, 64, 64, 32], P(None, 'gx', 'gy', 'gz'), may hold values from 0 to 16383, as said below
- counts: int32 [1, 64, 64, 64], P(None, 'gx', 'gy', 'gz'), may hold values from 1 to 32, as said below
- kernel_in: bfloat16 [6, 80], replicated, may hold values from -2.5 to 2.5
- kernel_mid: bfloat16 [80, 80], replicated, may hold values from -0.625 to 0.625
- kernel_out: bfloat16 [80, 64], replicated, may hold values from -0.625 to 0.625
- spectral: bfloat16 [2, 16, 16, 16, 64, 64], P(None, 'gz', 'gx', 'gy'), may hold values from -48 to 48
- skip_weight: bfloat16 [64, 64], replicated, may hold values from -0.75 to 0.75
Outputs:
- latent_out: float32 [1, 64, 64, 64, 64], P(None, 'gx', 'gy', 'gz')
The draws below stay inside these ranges and needn't reach their ends.
Inputs may be any that keep to these rules, and one draw needn't show every extreme that they name: `neighbours`: points are owned by location: point j of a geometry belongs to the device at position j // 512 in the order gx, gy, gz. Every neighbour of a node is owned by the node's own device or by a device whose gx, gy and gz indices each differ from it by at most one. Slots s >= counts of the node are padding that names some point all the same. `counts`: on every device some node of every geometry has all 32 slots valid.
All inputs are finite; a program needn't handle non-finite values.
Results may differ from the reference program's by a relative error of at most 0.02.
Values may be sent and summed in bfloat16 or wider, within the bound.
A program may use at most 128 MiB of HBM per device.

```python
import math
import jax
import jax.numpy as jnp
from jax import lax

GRID = 64
CH = 64
MODES = 16
KH = 80
NB = 32
PT_DEV = 512
GEOMS = 1
LX = 16
LY = 16
LZ = 32
POINTS = 16384


def draw_neighbours(key, part):
    code_key, slot_key = jax.random.split(jax.random.fold_in(key, 11))
    shape = (GEOMS, GRID, GRID, GRID, NB)
    codes = jax.random.randint(code_key, shape, 0, 54)
    codes = jnp.where(codes >= 27, 13, codes)
    count_x = GRID // LX
    count_y = GRID // LY
    count_z = GRID // LZ
    home_x = (jnp.arange(GRID, dtype=jnp.int32) // LX).reshape(1, GRID, 1, 1, 1)
    home_y = (jnp.arange(GRID, dtype=jnp.int32) // LY).reshape(1, 1, GRID, 1, 1)
    home_z = (jnp.arange(GRID, dtype=jnp.int32) // LZ).reshape(1, 1, 1, GRID, 1)
    owner_x = jnp.clip(home_x + codes // 9 - 1, 0, count_x - 1)
    owner_y = jnp.clip(home_y + codes // 3 % 3 - 1, 0, count_y - 1)
    owner_z = jnp.clip(home_z + codes % 3 - 1, 0, count_z - 1)
    slots = jax.random.randint(slot_key, shape, 0, PT_DEV)
    return (((owner_x * count_y + owner_y) * count_z + owner_z) * PT_DEV + slots).astype(jnp.int32)


def draw_counts(key, part):
    values = jax.random.randint(jax.random.fold_in(key, 12), (GEOMS, GRID, GRID, GRID), 1, NB + 1)
    return values.at[:, ::LX, ::LY, ::LZ].set(NB).astype(jnp.int32)


def block_scale(own_key, extent, cuts, low, high):
    def one(dim, parts):
        draws = jax.random.uniform(jax.random.fold_in(jax.random.fold_in(own_key, 6), dim), (parts,), jnp.float32, low / len(cuts), high / len(cuts))
        return jnp.repeat(jnp.exp(draws), extent[dim] // parts).reshape((-1,) + (1,) * (len(extent) - dim - 1))

    level = one(*cuts[0])
    for cut in cuts[1:]:
        level = level * one(*cut)
    return level


def normal_values(key, shape, deviation, most, pieces=(), kind=jnp.bfloat16):
    drawn = deviation * jax.random.normal(key, shape, jnp.float32)
    if pieces:
        drawn = drawn * block_scale(key, shape, pieces, -0.22, 0.18)
    return jnp.clip(drawn, -most, most).astype(kind)


def setup_inputs(seed: int = 0) -> dict:
    key_list = jax.random.split(jax.random.key(seed), 9)
    return {
        "point_data": jnp.clip(jax.random.uniform(key_list[0], (GEOMS, 6, POINTS), jnp.float32, -1.0, 1.0) * block_scale(key_list[0], (GEOMS, 6, POINTS), ((2, 32),), -0.4, 0.0), -1.0, 1.0),
        "neighbours": draw_neighbours(jax.random.fold_in(key_list[8], 71), 0),
        "counts": draw_counts(jax.random.fold_in(key_list[8], 71), 0),
        "kernel_in": normal_values(key_list[3], (6, KH), 6 ** -0.5, 2.5),
        "kernel_mid": normal_values(key_list[4], (KH, KH), KH ** -0.5, 0.625),
        "kernel_out": normal_values(key_list[5], (KH, CH), KH ** -0.5, 0.625),
        "spectral": normal_values(key_list[6], (2, MODES, MODES, MODES, CH, CH), 8.0, 48.0, ((1, 2), (2, 4), (3, 4))),
        "skip_weight": normal_values(key_list[7], (CH, CH), CH ** -0.5, 0.75),
    }


HIGHEST = lax.Precision.HIGHEST
NORM_FLOOR = 1.0

def tables(length, keep_count, centred):
    position = jnp.arange(length, dtype=jnp.int32)
    frequency = jnp.arange(keep_count, dtype=jnp.int32)
    if centred:
        frequency = jnp.where(frequency < keep_count // 2, frequency, frequency + length - keep_count)
    phases = frequency[:, None] * position[None, :] % length
    angles = phases.astype(jnp.float32) * (2.0 * math.pi / length)
    return (jnp.cos(angles), jnp.sin(angles))

def third_weights(cos_table, sin_table, length):
    factor = jnp.where(jnp.arange(cos_table.shape[0]) == 0, 1.0, 2.0).astype(jnp.float32)[:, None] / length ** 3
    return (cos_table * factor, sin_table * factor)

def contract(pattern, operand, table):
    return jnp.einsum(pattern, operand, table, precision=HIGHEST)

def forward_real(values, cos_table, sin_table, pattern):
    return (contract(pattern, values, cos_table), -contract(pattern, values, sin_table))

def forward_complex(real_part, imag_part, cos_table, sin_table, pattern):
    new_real = contract(pattern, real_part, cos_table) + contract(pattern, imag_part, sin_table)
    new_imag = contract(pattern, imag_part, cos_table) - contract(pattern, real_part, sin_table)
    return (new_real, new_imag)

def inverse_complex(real_part, imag_part, cos_table, sin_table, pattern):
    new_real = contract(pattern, real_part, cos_table) - contract(pattern, imag_part, sin_table)
    new_imag = contract(pattern, real_part, sin_table) + contract(pattern, imag_part, cos_table)
    return (new_real, new_imag)

def inverse_real(real_part, imag_part, cos_table, sin_table, pattern):
    return contract(pattern, real_part, cos_table) - contract(pattern, imag_part, sin_table)

def kernel_mean(pair, valid, kernel_in, kernel_mid, kernel_out):
    hidden_one = jax.nn.gelu(jnp.dot(kernel_in.T, pair, preferred_element_type=jnp.float32), approximate=True).astype(jnp.bfloat16)
    hidden_two = jax.nn.gelu(jnp.dot(kernel_mid.T, hidden_one, preferred_element_type=jnp.float32), approximate=True).astype(jnp.bfloat16)
    values = jnp.dot(kernel_out.T, hidden_two, preferred_element_type=jnp.float32)
    values = values.reshape(values.shape[0], -1, NB)
    slots = jnp.arange(NB, dtype=jnp.int32)
    used = (slots[None, :] < valid[:, None]).astype(jnp.float32)
    total = lax.optimization_barrier(jnp.sum(values * used[None], axis=2))
    return (total / valid.astype(jnp.float32)[None]).T.astype(jnp.bfloat16)

def reference(point_data, neighbours, counts, kernel_in, kernel_mid, kernel_out, spectral, skip_weight):
    centres = (jnp.arange(GRID, dtype=jnp.int32).astype(jnp.float32) + 0.5) / GRID
    row_y = jnp.broadcast_to(centres[:, None, None], (GRID, GRID, NB)).reshape(1, -1)
    row_z = jnp.broadcast_to(centres[None, :, None], (GRID, GRID, NB)).reshape(1, -1)

    def one_slab(step):
        geometry = step // GRID
        slab = step % GRID
        points = lax.dynamic_index_in_dim(point_data, geometry, 0, keepdims=False)
        near = lax.dynamic_index_in_dim(lax.dynamic_index_in_dim(neighbours, geometry, 0, keepdims=False), slab, 0, keepdims=False).reshape(-1)
        valid = lax.dynamic_index_in_dim(lax.dynamic_index_in_dim(counts, geometry, 0, keepdims=False), slab, 0, keepdims=False).reshape(-1)
        picked = jnp.take(points, near, axis=1)
        row_x = (slab.astype(jnp.float32) + 0.5) / GRID
        pair = jnp.concatenate([picked[0:1] - row_x, picked[1:2] - row_y, picked[2:3] - row_z, picked[3:6]], axis=0).astype(jnp.bfloat16)
        return kernel_mean(pair, valid, kernel_in, kernel_mid, kernel_out)
    latent = lax.map(one_slab, jnp.arange(GEOMS * GRID, dtype=jnp.int32)).reshape(GEOMS, GRID, GRID, GRID, CH)
    cos_centred, sin_centred = tables(GRID, MODES, True)
    cos_third, sin_third = tables(GRID, MODES, False)
    back_cos, back_sin = third_weights(cos_third, sin_third, GRID)
    latent_wide = latent.astype(jnp.float32)
    real_part, imag_part = forward_real(latent_wide, cos_third, sin_third, 'gxyzc,kz->gxykc')
    real_part, imag_part = forward_complex(real_part, imag_part, cos_centred, sin_centred, 'gxykc,jy->gxjkc')
    real_part, imag_part = forward_complex(real_part, imag_part, cos_centred, sin_centred, 'gxjkc,ix->gijkc')
    spec_real = lax.optimization_barrier(real_part.astype(jnp.bfloat16)).astype(jnp.float32)
    spec_imag = lax.optimization_barrier(imag_part.astype(jnp.bfloat16)).astype(jnp.float32)
    mix_real = spectral[0].astype(jnp.float32)
    mix_imag = spectral[1].astype(jnp.float32)
    mixed_real = jnp.einsum('gijkc,ijkco->gijko', spec_real, mix_real) - jnp.einsum('gijkc,ijkco->gijko', spec_imag, mix_imag)
    mixed_imag = jnp.einsum('gijkc,ijkco->gijko', spec_real, mix_imag) + jnp.einsum('gijkc,ijkco->gijko', spec_imag, mix_real)
    mixed_real = lax.optimization_barrier(mixed_real.astype(jnp.bfloat16)).astype(jnp.float32)
    mixed_imag = lax.optimization_barrier(mixed_imag.astype(jnp.bfloat16)).astype(jnp.float32)
    real_part, imag_part = inverse_complex(mixed_real, mixed_imag, cos_centred, sin_centred, 'gijkc,ix->gxjkc')
    real_part, imag_part = inverse_complex(real_part, imag_part, cos_centred, sin_centred, 'gxjkc,jy->gxykc')
    branch = inverse_real(real_part, imag_part, back_cos, back_sin, 'gxykc,kz->gxyzc')
    cells_total = float(GRID ** 3)
    mean = lax.optimization_barrier(jnp.sum(branch, axis=(1, 2, 3))) / cells_total
    centred_branch = branch - mean[:, None, None, None, :]
    variance = lax.optimization_barrier(jnp.sum(centred_branch * centred_branch, axis=(1, 2, 3))) / cells_total
    skip = jnp.dot(latent.reshape(-1, CH), skip_weight, preferred_element_type=jnp.float32).reshape(GEOMS, GRID, GRID, GRID, CH)
    normed = centred_branch / jnp.sqrt(variance + NORM_FLOOR)[:, None, None, None, :]
    return jax.nn.gelu(normed + skip, approximate=True)
```

```python
import functools
import math

import jax
import jax.numpy as jnp
from jax import lax
from jax.experimental import pallas as pl
from jax.experimental.pallas import tpu as pltpu
from jax.sharding import PartitionSpec as P

GRID = 64
MODES = 16
NB = 32


HIGH = lax.Precision.HIGH
NORM_FLOOR = 1.0


def beside(cells, axis, dim):
    count = lax.axis_size(axis)
    turn = lambda by: lax.ppermute(cells, axis, [(i, (i + by) % count) for i in range(count)])
    if count == 1:
        return cells
    if count == 2:
        return jnp.concatenate([cells, turn(1)], axis=dim)
    return jnp.concatenate([turn(1), cells, turn(-1)], axis=dim)


def offset(owner, axis):
    count = lax.axis_size(axis)
    return (owner - lax.axis_index(axis) + (1 if count > 2 else 0)) % count, min(count, 3)


def tables(length, keep_count, centred):
    position = jnp.arange(length, dtype=jnp.int32)
    frequency = jnp.arange(keep_count, dtype=jnp.int32)
    if centred:
        frequency = jnp.where(
            frequency < keep_count // 2, frequency, frequency + length - keep_count
        )
    phases = frequency[:, None] * position[None, :] % length
    angles = phases.astype(jnp.float32) * (2.0 * math.pi / length)
    return (jnp.cos(angles), jnp.sin(angles))


def third_weights(cos_table, sin_table, length):
    factor = (
        jnp.where(jnp.arange(cos_table.shape[0]) == 0, 1.0, 2.0).astype(jnp.float32)[:, None]
        / length**3
    )
    return (cos_table * factor, sin_table * factor)


def contract(pattern, operand, table):
    return jnp.einsum(pattern, operand, table, precision=HIGH)


def forward_real(values, cos_table, sin_table, pattern):
    return (contract(pattern, values, cos_table), -contract(pattern, values, sin_table))


def forward_complex(real_part, imag_part, cos_table, sin_table, pattern):
    new_real = contract(pattern, real_part, cos_table) + contract(pattern, imag_part, sin_table)
    new_imag = contract(pattern, imag_part, cos_table) - contract(pattern, real_part, sin_table)
    return (new_real, new_imag)


def inverse_complex(real_part, imag_part, cos_table, sin_table, pattern):
    new_real = contract(pattern, real_part, cos_table) - contract(pattern, imag_part, sin_table)
    new_imag = contract(pattern, real_part, sin_table) + contract(pattern, imag_part, cos_table)
    return (new_real, new_imag)


def inverse_real(real_part, imag_part, cos_table, sin_table, pattern):
    return contract(pattern, real_part, cos_table) - contract(pattern, imag_part, sin_table)


SUB = 8
LANES = 128

SCALE = 0.035677408136300125 ** (-1.0 / 3.0)
SHIFT = 0.7978845608028654 * SCALE

def gelu2(y):
    return y + y * jnp.tanh(y * (y * y + jnp.asarray(SHIFT, y.dtype)))

def pick(leaf, bits, low, high, level):
    if high - low == 1:
        return leaf(low)
    half = 1 << (level - 1)
    if low + half >= high:
        return pick(leaf, bits, low, high, level - 1)
    a = pick(leaf, bits, low, low + half, level - 1)
    b = pick(leaf, bits, low + half, high, level - 1)
    return jnp.where(bits[level - 1], b, a)

def encoder_kernel(codes_ref, counts_ref, centres_ref, table_ref, first_ref, mid_ref, last_ref, out_ref, acc_ref, dt=jnp.bfloat16, per=2):
    slots, rows = codes_ref.shape[0:2]
    groups = rows // SUB
    words, table_rows = table_ref.shape[0:2]
    units = mid_ref.shape[0]
    channels = last_ref.shape[0]
    depth = max(1, (table_rows - 1).bit_length())
    acc_ref[...] = jnp.zeros_like(acc_ref)
    counts = [counts_ref[SUB*g:SUB*(g+1), :] for g in range(groups)]
    scale = 1.0 / (32767.0 * SCALE)
    def pairs(i):
        out = []
        for k in range(per):
            s = i * per + k
            stacks = []
            for g in range(groups):
                code = codes_ref[s, SUB*g:SUB*(g+1), :]
                lane = code & (LANES - 1)
                bits = [(code & (LANES << b)) != 0 for b in range(depth)]
                live = s < counts[g]
                vals = []
                for w in range(words):
                    leaf = lambda r: jnp.take_along_axis(
                        jnp.broadcast_to(table_ref[w, r:r+1, :], (SUB, LANES)), lane, axis=1, mode="promise_in_bounds")
                    word = pick(leaf, bits, 0, table_rows, depth)
                    vals += [word >> 16, (word & 65535) - 32768]
                parts = []
                for v in range(6):
                    x = vals[v].astype(jnp.float32) * scale
                    if v < 3:
                        x = x - centres_ref[v, SUB*g:SUB*(g+1), :]
                    parts.append(jnp.where(live, x, 0.0))
                stacks.append(jnp.concatenate(parts, axis=0).astype(jnp.bfloat16))
            out.append(jnp.concatenate(stacks, axis=1))
        return out
    def step(i, stacks):
        h2s = []
        for k in range(per):
            z1 = jnp.dot(first_ref[...], stacks[k], preferred_element_type=jnp.float32)
            h1 = gelu2(z1.astype(dt)).astype(jnp.bfloat16)
            wide = jnp.concatenate([h1[units*r:units*(r+1)] for r in range(SUB)], axis=1)
            z2 = jnp.dot(mid_ref[...], wide, preferred_element_type=jnp.float32)
            h2s.append(gelu2(z2.astype(dt)).astype(jnp.bfloat16))
        hidden = jnp.concatenate(h2s, axis=0)
        acc_ref[...] += jnp.dot(last_ref[...], hidden, preferred_element_type=jnp.float32)
        return pairs(jnp.minimum(i + 1, slots // per - 1))
    lax.fori_loop(0, slots // per, step, pairs(0))
    for r in range(SUB):
        for g in range(groups):
            at = (r * groups + g) * LANES
            row = SUB * g + r
            out_ref[row] = acc_ref[:, at:at+LANES] * SCALE / counts_ref[row:row+1, :].astype(jnp.float32)

def encode(codes, counts, centres, table, kernel_in, kernel_mid, kernel_out, dt=jnp.bfloat16, per=2):
    slots, rows = codes.shape[0:2]
    units, channels = kernel_out.shape
    block = min(16, rows)
    w1 = kernel_in.T.astype(jnp.float32)
    first = jnp.einsum("hv,rq->rhvq", w1, jnp.eye(SUB, dtype=jnp.float32)).reshape(SUB*units, 6*SUB).astype(jnp.bfloat16)
    mid = (kernel_mid.T * 0.5).astype(jnp.bfloat16)
    last = jnp.concatenate([(kernel_out.T * 0.5).astype(jnp.bfloat16)]*per, axis=1)
    whole = lambda a: pl.BlockSpec(a.shape, lambda i: (0,)*a.ndim)
    return pl.pallas_call(
        functools.partial(encoder_kernel, dt=dt, per=per),
        grid=(rows // block,),
        out_shape=jax.ShapeDtypeStruct((rows, channels, LANES), jnp.float32),
        in_specs=[pl.BlockSpec((slots, block, LANES), lambda i: (0, i, 0)),
                  pl.BlockSpec((block, LANES), lambda i: (i, 0)),
                  pl.BlockSpec((3, block, LANES), lambda i: (0, i, 0)),
                  whole(table), whole(first), whole(mid), whole(last)],
        out_specs=pl.BlockSpec((block, channels, LANES), lambda i: (i, 0, 0)),
        scratch_shapes=[pltpu.VMEM((channels, block*LANES), jnp.float32)],
    )(codes, counts, centres, table, first, mid, last)

def pack_table(points):
    q = jnp.round(points * 32767.0).astype(jnp.int32)
    word = q[0::2] * 65536 + (q[1::2] + 32768)
    return word.reshape(3, -1, LANES)


def summed_over_axes(values, axes):
    for axis in axes:
        count = lax.axis_size(axis)
        copies = jnp.broadcast_to(values[None], (count,) + values.shape)
        values = jnp.sum(lax.all_to_all(copies, axis, 0, 0, tiled=True), axis=0)
    return values


def exchange(values, axis, split_axis, concat_axis):
    return lax.all_to_all(
        values.astype(jnp.bfloat16), axis, split_axis=split_axis, concat_axis=concat_axis, tiled=True
    ).astype(jnp.float32)


def body(point_data, neighbours, counts, kernel_in, kernel_mid, kernel_out, spectral, skip_weight):
    count_y = lax.axis_size("gy")
    count_z = lax.axis_size("gz")
    place_x = lax.axis_index("gx")
    place_y = lax.axis_index("gy")
    place_z = lax.axis_index("gz")
    geometry_count, cells_x, cells_y, cells_z = neighbours.shape[0:4]
    per_device = point_data.shape[2]
    channels = skip_weight.shape[0]
    cells = point_data[:, :, None, None, None]
    for dim, axis in enumerate(("gx", "gy", "gz")):
        cells = beside(cells, axis, dim + 2)
    table = cells.reshape(geometry_count, point_data.shape[1], -1)
    owner = neighbours // per_device
    offset_z, width_z = offset(owner % count_z, "gz")
    offset_y, width_y = offset(owner // count_z % count_y, "gy")
    offset_x, _ = offset(owner // (count_z * count_y), "gx")
    block_index = (offset_x * width_y + offset_y) * width_z + offset_z
    slot_index = neighbours % per_device
    centre_y = (
        (place_y * cells_y + jnp.arange(cells_y, dtype=jnp.int32)).astype(jnp.float32) + 0.5
    ) / GRID
    centre_z = (
        (place_z * cells_z + jnp.arange(cells_z, dtype=jnp.int32)).astype(jnp.float32) + 0.5
    ) / GRID
    centre_x = (
        (place_x * cells_x + jnp.arange(cells_x, dtype=jnp.int32)).astype(jnp.float32) + 0.5
    ) / GRID
    shape = (cells_x, cells_y, cells_z)
    centres = jnp.stack(
        [
            jnp.broadcast_to(centre_x[:, None, None], shape).reshape(-1),
            jnp.broadcast_to(centre_y[None, :, None], shape).reshape(-1),
            jnp.broadcast_to(centre_z[None, None, :], shape).reshape(-1),
        ]
    )
    centres = (centres / SCALE).reshape(3, -1, LANES)
    code = (block_index * per_device + slot_index).reshape(geometry_count, -1, NB)
    latent = []
    for geometry in range(geometry_count):
        turned = code[geometry].T.reshape(NB, -1, LANES)
        latent.append(
            encode(
                turned,
                counts[geometry].reshape(-1, LANES),
                centres,
                pack_table(table[geometry]),
                kernel_in,
                kernel_mid,
                kernel_out,
            )
        )
    latent = jnp.swapaxes(jnp.stack(latent), 2, 3).astype(jnp.bfloat16)
    latent = latent.reshape(geometry_count, cells_x, cells_y, cells_z, channels)
    cos_centred, sin_centred = tables(GRID, MODES, True)
    cos_third, sin_third = tables(GRID, MODES, False)
    back_cos, back_sin = third_weights(cos_third, sin_third, GRID)
    depth_full = lax.all_to_all(latent, "gz", split_axis=4, concat_axis=3, tiled=True)
    real_part, imag_part = forward_real(
        depth_full.astype(jnp.float32), cos_third, sin_third, "gxyzc,kz->gxykc"
    )
    real_part, imag_part = (
        lax.all_to_all(real_part, "gy", split_axis=3, concat_axis=2, tiled=True),
        lax.all_to_all(imag_part, "gy", split_axis=3, concat_axis=2, tiled=True),
    )
    real_part, imag_part = forward_complex(
        real_part, imag_part, cos_centred, sin_centred, "gxykc,jy->gxjkc"
    )
    real_part, imag_part = (
        lax.all_to_all(real_part, "gx", split_axis=2, concat_axis=1, tiled=True),
        lax.all_to_all(imag_part, "gx", split_axis=2, concat_axis=1, tiled=True),
    )
    real_part, imag_part = forward_complex(
        real_part, imag_part, cos_centred, sin_centred, "gxjkc,ix->gijkc"
    )
    spec_real, spec_imag = (
        exchange(real_part, "gz", split_axis=1, concat_axis=4),
        exchange(imag_part, "gz", split_axis=1, concat_axis=4),
    )
    spec_real = spec_real.astype(jnp.bfloat16)
    spec_imag = spec_imag.astype(jnp.bfloat16)
    mixed_real = jnp.einsum(
        "gijkc,ijkco->gijko", spec_real, spectral[0], preferred_element_type=jnp.float32
    ) - jnp.einsum("gijkc,ijkco->gijko", spec_imag, spectral[1], preferred_element_type=jnp.float32)
    mixed_imag = jnp.einsum(
        "gijkc,ijkco->gijko", spec_real, spectral[1], preferred_element_type=jnp.float32
    ) + jnp.einsum("gijkc,ijkco->gijko", spec_imag, spectral[0], preferred_element_type=jnp.float32)
    first_place = (place_x + place_y + place_z) == 0
    modes = mixed_real.shape[1:4]
    order = sum(lax.broadcasted_iota(jnp.int32, modes, d) for d in range(3))
    zero_mode = ((order == 0) & first_place)[None, ..., None]
    mixed_real = jnp.where(zero_mode, 0.0, mixed_real)
    mixed_imag = jnp.where(zero_mode, 0.0, mixed_imag)
    mixed_real = mixed_real.astype(jnp.bfloat16)
    mixed_imag = mixed_imag.astype(jnp.bfloat16)
    real_part, imag_part = (
        exchange(mixed_real, "gz", split_axis=4, concat_axis=1),
        exchange(mixed_imag, "gz", split_axis=4, concat_axis=1),
    )
    real_part, imag_part = inverse_complex(
        real_part.astype(jnp.float32),
        imag_part.astype(jnp.float32),
        cos_centred,
        sin_centred,
        "gijkc,ix->gxjkc",
    )
    real_part, imag_part = (
        exchange(real_part, "gx", split_axis=1, concat_axis=2),
        exchange(imag_part, "gx", split_axis=1, concat_axis=2),
    )
    real_part, imag_part = inverse_complex(
        real_part, imag_part, cos_centred, sin_centred, "gxjkc,jy->gxykc"
    )
    real_part, imag_part = (
        exchange(real_part, "gy", split_axis=2, concat_axis=3),
        exchange(imag_part, "gy", split_axis=2, concat_axis=3),
    )
    depth_part = inverse_real(real_part, imag_part, back_cos, back_sin, "gxykc,kz->gxyzc")
    branch = exchange(depth_part, "gz", split_axis=3, concat_axis=4)
    skip = jnp.einsum("gxyzc,co->gxyzo", latent, skip_weight, preferred_element_type=jnp.float32)
    cells_total = float(GRID**3)
    variance = (
        summed_over_axes(jnp.sum(branch * branch, axis=(1, 2, 3)), ("gz", "gy", "gx")) / cells_total
    )
    normed = branch / jnp.sqrt(variance + NORM_FLOOR)[:, None, None, None, :]
    return jax.nn.gelu(normed + skip, approximate=True)


def solution(mesh):
    in_specs = (
        P(None, None, ("gx", "gy", "gz")),
        P(None, "gx", "gy", "gz", None),
        P(None, "gx", "gy", "gz"),
        P(),
        P(),
        P(),
        P(None, "gz", "gx", "gy", None, None),
        P(),
    )
    out_specs = P(None, "gx", "gy", "gz", None)
    return jax.shard_map(body, mesh=mesh, in_specs=in_specs, out_specs=out_specs, check_vma=False)
```

```python
import functools
import math

import jax
import jax.numpy as jnp
import numpy as np
from jax import lax
from jax.experimental import pallas as pl
from jax.experimental.pallas import tpu as pltpu
from jax.sharding import PartitionSpec as P

GRID = 64
MODES = 16
NB = 32


HIGH = lax.Precision.HIGH
NORM_FLOOR = 1.0


def beside(cells, axis, dim):
    count = lax.axis_size(axis)
    turn = lambda by: lax.ppermute(cells, axis, [(i, (i + by) % count) for i in range(count)])
    if count == 1:
        return cells
    if count == 2:
        return jnp.concatenate([cells, turn(1)], axis=dim)
    return jnp.concatenate([turn(1), cells, turn(-1)], axis=dim)


def offset(owner, axis):
    count = lax.axis_size(axis)
    return (owner - lax.axis_index(axis) + (1 if count > 2 else 0)) % count, min(count, 3)


def tables(length, keep_count, centred):
    position = jnp.arange(length, dtype=jnp.int32)
    frequency = jnp.arange(keep_count, dtype=jnp.int32)
    if centred:
        frequency = jnp.where(
            frequency < keep_count // 2, frequency, frequency + length - keep_count
        )
    phases = frequency[:, None] * position[None, :] % length
    angles = phases.astype(jnp.float32) * (2.0 * math.pi / length)
    return (jnp.cos(angles), jnp.sin(angles))


def third_weights(cos_table, sin_table, length):
    factor = (
        jnp.where(jnp.arange(cos_table.shape[0]) == 0, 1.0, 2.0).astype(jnp.float32)[:, None]
        / length**3
    )
    return (cos_table * factor, sin_table * factor)


def contract(pattern, operand, table):
    return jnp.einsum(pattern, operand, table, precision=HIGH)


def forward_real(values, cos_table, sin_table, pattern):
    return (contract(pattern, values, cos_table), -contract(pattern, values, sin_table))


def forward_complex(real_part, imag_part, cos_table, sin_table, pattern):
    new_real = contract(pattern, real_part, cos_table) + contract(pattern, imag_part, sin_table)
    new_imag = contract(pattern, imag_part, cos_table) - contract(pattern, real_part, sin_table)
    return (new_real, new_imag)


def inverse_complex(real_part, imag_part, cos_table, sin_table, pattern):
    new_real = contract(pattern, real_part, cos_table) - contract(pattern, imag_part, sin_table)
    new_imag = contract(pattern, real_part, sin_table) + contract(pattern, imag_part, cos_table)
    return (new_real, new_imag)


def inverse_real(real_part, imag_part, cos_table, sin_table, pattern):
    return contract(pattern, real_part, cos_table) - contract(pattern, imag_part, sin_table)


SUB = 8
LANES = 128

SCALE = 0.035677408136300125 ** (-1.0 / 3.0)
SHIFT = 0.7978845608028654 * SCALE

def gelu2(y):
    return y + y * jnp.tanh(y * (y * y + jnp.asarray(SHIFT, y.dtype)))

def pick(leaf, bits, low, high, level):
    if high - low == 1:
        return leaf(low)
    half = 1 << (level - 1)
    if low + half >= high:
        return pick(leaf, bits, low, high, level - 1)
    a = pick(leaf, bits, low, low + half, level - 1)
    b = pick(leaf, bits, low + half, high, level - 1)
    return jnp.where(bits[level - 1], b, a)

def encoder_kernel(codes_ref, counts_ref, centres_ref, table_ref, first_ref, mid_ref, last_ref, out_ref, acc_ref, grouped, dt=jnp.bfloat16, per=2):
    slots, rows = codes_ref.shape[0:2]
    groups = rows // SUB
    words, table_rows = table_ref.shape[0:2]
    units = mid_ref.shape[0]
    channels = last_ref.shape[0]
    depth = max(1, (table_rows - 1).bit_length())
    acc_ref[...] = jnp.zeros_like(acc_ref)
    counts = [counts_ref[SUB*g:SUB*(g+1), :] for g in range(groups)]
    scale = 1.0 / (32767.0 * SCALE)
    def pairs(i):
        out = []
        for k in range(per):
            s = i * per + k
            stacks = []
            for g in range(groups):
                code = codes_ref[s, SUB*g:SUB*(g+1), :]
                lane = code & (LANES - 1)
                bits = [(code & (LANES << b)) != 0 for b in range(depth)]
                live = s < counts[g]
                vals = []
                for w in range(words):
                    leaf = lambda r: jnp.take_along_axis(
                        jnp.broadcast_to(table_ref[w, r:r+1, :], (SUB, LANES)), lane, axis=1, mode="promise_in_bounds")
                    word = pick(leaf, bits, 0, table_rows, depth)
                    vals += [word >> 16, (word & 65535) - 32768]
                parts = []
                for v in range(6):
                    x = vals[v].astype(jnp.float32) * scale
                    if v < 3:
                        x = x - centres_ref[v, SUB*g:SUB*(g+1), :]
                    parts.append(jnp.where(live, x, 0.0))
                stacks.append(jnp.concatenate(parts, axis=0).astype(jnp.bfloat16))
            out.append(jnp.concatenate(stacks, axis=1))
        return out
    def step(i, stacks):
        h2s = []
        for k in range(per):
            z1 = jnp.dot(first_ref[...], stacks[k], preferred_element_type=jnp.float32)
            h1 = gelu2(z1.astype(dt)).astype(jnp.bfloat16)
            wide = jnp.concatenate([h1[units*r:units*(r+1)] for r in range(SUB)], axis=1)
            z2 = jnp.dot(mid_ref[...], wide, preferred_element_type=jnp.float32)
            h2s.append(gelu2(z2.astype(dt)).astype(jnp.bfloat16))
        hidden = jnp.concatenate(h2s, axis=0)
        acc_ref[...] += jnp.dot(last_ref[...], hidden, preferred_element_type=jnp.float32)
        return pairs(jnp.minimum(i + 1, slots // per - 1))
    lax.fori_loop(0, slots // per, step, pairs(0))
    done = {}
    for r in range(SUB):
        for g in range(groups):
            at = (r * groups + g) * LANES
            row = SUB * g + r
            done[row] = acc_ref[:, at:at+LANES] * SCALE / counts_ref[row:row+1, :].astype(jnp.float32)
            if not grouped:
                out_ref[row] = done[row]
    if grouped:
        for q in range(channels // SUB):
            out_ref[q] = jnp.concatenate(
                [done[row][SUB * q : SUB * (q + 1)] for row in range(rows)], axis=0
            ).astype(jnp.bfloat16)

def encode(codes, counts, centres, table, kernel_in, kernel_mid, kernel_out, grouped, dt=jnp.bfloat16, per=2):
    slots, rows = codes.shape[0:2]
    units, channels = kernel_out.shape
    block = min(16, rows)
    w1 = kernel_in.T.astype(jnp.float32)
    first = jnp.einsum("hv,rq->rhvq", w1, jnp.eye(SUB, dtype=jnp.float32)).reshape(SUB*units, 6*SUB).astype(jnp.bfloat16)
    mid = (kernel_mid.T * 0.5).astype(jnp.bfloat16)
    last = jnp.concatenate([(kernel_out.T * 0.5).astype(jnp.bfloat16)]*per, axis=1)
    whole = lambda a: pl.BlockSpec(a.shape, lambda i: (0,)*a.ndim)
    if grouped:
        shape = jax.ShapeDtypeStruct((channels // SUB, rows * SUB, LANES), jnp.bfloat16)
        out_spec = pl.BlockSpec((channels // SUB, block * SUB, LANES), lambda i: (0, i, 0))
    else:
        shape = jax.ShapeDtypeStruct((rows, channels, LANES), jnp.float32)
        out_spec = pl.BlockSpec((block, channels, LANES), lambda i: (i, 0, 0))
    return pl.pallas_call(
        functools.partial(encoder_kernel, grouped=grouped, dt=dt, per=per),
        grid=(rows // block,),
        out_shape=shape,
        in_specs=[pl.BlockSpec((slots, block, LANES), lambda i: (0, i, 0)),
                  pl.BlockSpec((block, LANES), lambda i: (i, 0)),
                  pl.BlockSpec((3, block, LANES), lambda i: (0, i, 0)),
                  whole(table), whole(first), whole(mid), whole(last)],
        out_specs=out_spec,
        scratch_shapes=[pltpu.VMEM((channels, block*LANES), jnp.float32)],
    )(codes, counts, centres, table, first, mid, last)

def pack_table(points):
    q = jnp.round(points * 32767.0).astype(jnp.int32)
    word = q[0::2] * 65536 + (q[1::2] + 32768)
    return word.reshape(3, -1, LANES)


def lane_maps(quarters, parts, inner_k, inner_j):
    grid = np.indices((quarters, 2, parts, inner_k, inner_j)).reshape(5, -1)
    return grid[0] * inner_j + grid[4], grid[2] * inner_k + grid[3], grid[1]


def spectral_tables(count_x, count_y, count_z, cells_x, cells_y, cells_z, group):
    keep = MODES
    signed = np.where(np.arange(keep) < keep // 2, np.arange(keep), np.arange(keep) - keep)
    mode_j, mode_k, imaginary = lane_maps(count_x, count_y, keep // count_y, keep // count_x)
    turn = 2.0 * np.pi / GRID
    rows_y = LANES // cells_z
    place_z, row_y, cell_z = np.indices((count_z, rows_y, cells_z)).reshape(3, -1)
    phase = turn * (
        (signed[mode_j] * row_y[:, None] + mode_k * (place_z * cells_z + cell_z)[:, None]) % GRID
    )
    forward = np.where(imaginary, -np.sin(phase), np.cos(phase))
    weight = np.where(mode_k == 0, 1.0, 2.0)
    inverse = (np.where(imaginary, -np.sin(phase), np.cos(phase)) * weight).T
    sign = np.where(imaginary, -1.0, 1.0)
    strip = turn * ((signed[mode_j] * (rows_y * np.arange(GRID // rows_y))[:, None]) % GRID)
    strips = np.stack([np.cos(strip), np.sin(strip) * sign])
    cell = np.arange(count_x * cells_x).reshape(count_x, 1, cells_x)
    angle = turn * ((signed[:, None] * cell) % GRID)
    eye = np.eye(group)

    def expand(values):
        wide = np.einsum("pab,cd->pacbd", values, eye)
        return wide.reshape(count_x, values.shape[1] * group, values.shape[2] * group)

    ahead = np.concatenate([expand(np.cos(angle)), expand(np.sin(angle))], axis=2)
    back = np.swapaxes(angle, 1, 2)
    back = np.concatenate([expand(np.cos(back)), expand(np.sin(back))], axis=2)
    partner = (keep - mode_j) % keep
    same = (
        (mode_j[:, None] == partner[None, :])
        & (mode_k[:, None] == 0)
        & (mode_k[None, :] == 0)
        & (imaginary[:, None] == imaginary[None, :])
        & (mode_j[:, None] != keep // 2)
    )
    flip = same * sign[None, :]
    power = np.where(mode_k == 0, 0.5, 2.0)
    lanes = np.stack([sign, power])
    narrow = lambda array: jnp.asarray(array.astype(np.float32), jnp.bfloat16)
    single = lambda array: jnp.asarray(array.astype(np.float32))
    return (
        narrow(forward),
        narrow(inverse),
        single(strips),
        narrow(ahead),
        narrow(back),
        narrow(flip),
        single(lanes),
    )


def swap_halves(values):
    return jnp.concatenate(
        [
            pltpu.roll(values[:, at : at + LANES], LANES // 2, 1)
            for at in range(0, values.shape[1], LANES)
        ],
        axis=1,
    )


def split(values):
    upper = values.astype(jnp.bfloat16)
    return upper, (values - upper.astype(jnp.float32)).astype(jnp.bfloat16)


def spectral_kernel(
    count_x,
    count_y,
    count_z,
    lat_ref,
    weight_ref,
    forward_ref,
    inverse_ref,
    strips_ref,
    ahead_ref,
    back_ref,
    flip_ref,
    lanes_ref,
    out_ref,
    came,
    plane,
    sums,
    sums_in,
    own,
    own_in,
    turned,
    mixed,
    mixed_in,
    joined,
    all_modes,
    pieces,
    send_a, recv_a, send_b, recv_b, send_c, recv_c, send_d, recv_d, send_e, recv_e, send_f, recv_f,
):
    place_x, place_y, place_z = lax.axis_index("gx"), lax.axis_index("gy"), lax.axis_index("gz")
    members = count_y * count_z
    me = place_y * count_z + place_z
    group = SUB
    strip_rows = plane.shape[0]
    half_modes = MODES // count_z
    inner = (MODES // count_x) * (MODES // count_y)
    mesh_id = pl.DeviceIdType.MESH

    def member(t):
        other = lax.rem(me + t, members)
        return other, {"gy": other // count_z, "gz": lax.rem(other, count_z)}

    def column(t):
        other = lax.rem(place_x + t, count_x)
        return other, {"gx": other}

    barrier = pltpu.get_barrier_semaphore()
    for t in range(1, members):
        pl.semaphore_signal(barrier, inc=1, device_id=member(t)[1], device_id_type=mesh_id)
    for t in range(1, count_x):
        pl.semaphore_signal(barrier, inc=1, device_id=column(t)[1], device_id_type=mesh_id)
    pl.semaphore_wait(barrier, members - 1 + count_x - 1)

    def exchange_with(peer, total, source, target, send, recv):
        copies = []
        for t in range(1, total):
            other, device = peer(t)
            copy = pltpu.make_async_remote_copy(
                src_ref=source(other),
                dst_ref=target,
                send_sem=send.at[t],
                recv_sem=recv.at[t],
                device_id=device,
                device_id_type=mesh_id,
            )
            copy.start()
            copies.append(copy)
        return copies

    copies = exchange_with(member, members, lambda p: lat_ref.at[p], came.at[me], send_a, recv_a)
    came[me] = lat_ref[me]
    sign = lanes_ref[0:1, :]
    plane[...] = jnp.zeros_like(plane)
    for copy in copies:
        copy.wait()

    strips = GRID // (came.shape[1] // strip_rows * count_y)
    chunks = came.shape[1] // strip_rows
    strips = chunks * count_y

    def ahead_step(strip, carry):
        source = strip // chunks
        at = pl.multiple_of(lax.rem(strip, chunks) * strip_rows, strip_rows)
        block = jnp.concatenate(
            [came[source * count_z + z, pl.ds(at, strip_rows), :] for z in range(count_z)], axis=1
        )
        part = jnp.dot(block, forward_ref[...], preferred_element_type=jnp.float32)
        cosine = strips_ref[0, pl.ds(strip, 1), :]
        sine = strips_ref[1, pl.ds(strip, 1), :]
        plane[...] += part * cosine + swap_halves(part) * sine
        return carry

    lax.fori_loop(0, strips, ahead_step, 0)
    whole = plane[...]
    whole_high, whole_low = split(whole)
    turn_high, turn_low = split(swap_halves(whole) * sign)
    table = ahead_ref[place_x]
    total = jnp.dot(
        table, jnp.concatenate([whole_high, turn_high], axis=0), preferred_element_type=jnp.float32
    ) + jnp.dot(
        table, jnp.concatenate([whole_low, turn_low], axis=0), preferred_element_type=jnp.float32
    )
    for q in range(count_x):
        sums[q] = total[:, LANES * q : LANES * (q + 1)]
    copies = exchange_with(column, count_x, lambda p: sums.at[p], sums_in.at[place_x], send_b, recv_b)
    sums_in[place_x] = sums[place_x]
    for copy in copies:
        copy.wait()
    spectrum = sums_in[0]
    for q in range(1, count_x):
        spectrum = spectrum + sums_in[q]
    half_rows = half_modes * group
    for z in range(count_z):
        own[z] = spectrum[half_rows * z : half_rows * (z + 1)].astype(jnp.bfloat16)

    copies = exchange_with(
        member, members, lambda p: own.at[lax.rem(p, count_z)], own_in.at[me], send_c, recv_c
    )
    own_in[me] = own[place_z]
    mixed_rows = lax.broadcasted_iota(jnp.int32, (2 * inner, LANES), 0) % inner
    mixed_lanes = lax.broadcasted_iota(jnp.int32, (2 * inner, LANES), 1) // (LANES // 2)
    modes_j = MODES // count_x
    modes_k = MODES // count_y
    row_mode = (mixed_rows % modes_j) * modes_k + mixed_rows // modes_j
    first_place = (place_x + place_y + place_z) == 0
    mode_zero = lax.broadcasted_iota(jnp.int32, (inner, LANES // 2), 0) == 0
    turned[...] = jnp.zeros_like(turned)
    for copy in copies:
        copy.wait()
    arrived = [own_in[p].astype(jnp.float32) for p in range(members)]
    for i in range(half_modes):
        column_values = jnp.concatenate([a[group * i : group * (i + 1)] for a in arrived], axis=0)
        column_values = jnp.concatenate([column_values, column_values], axis=0)
        mixed[i] = column_values.T
        at = pl.multiple_of(place_y * inner, inner)
        both = jnp.concatenate(
            [mixed[i, pl.ds(at, inner), :], mixed[i, pl.ds(LANES // 2 + at, inner), :]], axis=0
        )
        wide = jnp.concatenate(
            [
                jnp.where(row_mode == 2 * t + mixed_lanes, both, 0.0).astype(jnp.bfloat16)
                for t in range(inner // 2)
            ],
            axis=1,
        )
        by_real = jnp.dot(wide, weight_ref[0, i], preferred_element_type=jnp.float32)
        by_imag = jnp.dot(wide, weight_ref[1, i], preferred_element_type=jnp.float32)
        real = by_real[:inner] - by_imag[inner:]
        imag = by_imag[:inner] + by_real[inner:]
        if i == 0:
            drop = jnp.logical_and(mode_zero, first_place)
            real = jnp.where(drop, 0.0, real)
            imag = jnp.where(drop, 0.0, imag)
        turned[i, pl.ds(at, inner), 0 : LANES // 2] = real
        turned[i, pl.ds(LANES // 2 + at, inner), 0 : LANES // 2] = imag
    flat = [turned[i].T for i in range(half_modes)]
    for p in range(members):
        joined[p] = jnp.concatenate(
            [f[group * p : group * (p + 1)] for f in flat], axis=0
        ).astype(jnp.bfloat16)

    copies = exchange_with(member, members, lambda p: joined.at[p], mixed_in.at[me], send_d, recv_d)
    mixed_in[me] = joined[me]
    for copy in copies:
        copy.wait()
    parts = []
    for z in range(count_z):
        value = mixed_in[z].astype(jnp.float32)
        for y in range(1, count_y):
            value = value + mixed_in[y * count_z + z].astype(jnp.float32)
        parts.append(value)
    all_modes[place_x] = jnp.concatenate(parts, axis=0).astype(jnp.bfloat16)
    copies = exchange_with(
        column, count_x, lambda p: all_modes.at[place_x], all_modes.at[place_x], send_e, recv_e
    )
    for copy in copies:
        copy.wait()
    modes = jnp.concatenate([all_modes[q] for q in range(count_x)], axis=1)
    scaled = modes.astype(jnp.float32) * (1.0 / GRID**3)
    partner = jnp.dot(modes, flip_ref[...], preferred_element_type=jnp.float32) * (1.0 / GRID**3)
    energy = None
    for i in range(MODES):
        value = scaled[group * i : group * (i + 1)]
        term = value * value * lanes_ref[1:2, :]
        if i != MODES // 2:
            other = (MODES - i) % MODES
            term = term + 0.5 * value * partner[group * other : group * (other + 1)]
        energy = term if energy is None else energy + term
    variance = jnp.sum(energy, axis=1, keepdims=True)
    gain = 1.0 / jnp.sqrt(variance + NORM_FLOOR)
    rotated = (swap_halves(scaled * float(GRID**3)) * -sign).astype(jnp.bfloat16)
    back = jnp.dot(
        back_ref[place_x], jnp.concatenate([modes, rotated], axis=0), preferred_element_type=jnp.float32
    )
    back = back.reshape(-1, group, back.shape[1]) * (gain * (1.0 / GRID**3))[None]
    plane[...] = back.reshape(plane.shape)

    def back_step(strip, carry):
        source = strip // chunks
        at = pl.multiple_of(lax.rem(strip, chunks) * strip_rows, strip_rows)
        cosine = strips_ref[0, pl.ds(strip, 1), :]
        sine = strips_ref[1, pl.ds(strip, 1), :]
        value = plane[...]
        value = (value * cosine - swap_halves(value) * sine).astype(jnp.bfloat16)
        result = jnp.dot(value, inverse_ref[...], preferred_element_type=jnp.float32)
        for z in range(count_z):
            pieces[source * count_z + z, pl.ds(at, strip_rows), :] = result[
                :, LANES * z : LANES * (z + 1)
            ].astype(jnp.bfloat16)
        return carry

    lax.fori_loop(0, strips, back_step, 0)
    copies = exchange_with(member, members, lambda p: pieces.at[p], out_ref.at[me], send_f, recv_f)
    out_ref[me] = pieces[me]
    for copy in copies:
        copy.wait()


def spectral_branch(lat, spectral):
    count_x, count_y, count_z = (lax.axis_size(a) for a in ("gx", "gy", "gz"))
    members, piece_rows, _ = lat.shape
    cells_x, cells_y, cells_z = GRID // count_x, GRID // count_y, GRID // count_z
    strip_rows = cells_x * SUB
    half_modes = MODES // count_z
    channels = spectral.shape[-1]
    inner = (MODES // count_x) * (MODES // count_y)
    lanes = 2 * MODES * MODES
    tables = spectral_tables(count_x, count_y, count_z, cells_x, cells_y, cells_z, SUB)
    weight = spectral.reshape(2, half_modes, inner * channels, channels)
    vmem = lambda: pl.BlockSpec(memory_space=pltpu.VMEM)
    half = half_modes * SUB
    dma = pltpu.SemaphoreType.DMA
    return pl.pallas_call(
        functools.partial(spectral_kernel, count_x, count_y, count_z),
        out_shape=jax.ShapeDtypeStruct(lat.shape, jnp.bfloat16),
        in_specs=[vmem() for _ in range(9)],
        out_specs=vmem(),
        scratch_shapes=[
            pltpu.VMEM(lat.shape, jnp.bfloat16),
            pltpu.VMEM((strip_rows, lanes), jnp.float32),
            pltpu.VMEM((count_x, MODES * SUB, LANES), jnp.float32),
            pltpu.VMEM((count_x, MODES * SUB, LANES), jnp.float32),
            pltpu.VMEM((count_z, half, LANES), jnp.bfloat16),
            pltpu.VMEM((members, half, LANES), jnp.bfloat16),
            pltpu.VMEM((half_modes, LANES, LANES), jnp.float32),
            pltpu.VMEM((half_modes, LANES, LANES), jnp.float32),
            pltpu.VMEM((members, half, LANES), jnp.bfloat16),
            pltpu.VMEM((members, half, LANES), jnp.bfloat16),
            pltpu.VMEM((count_x, MODES * SUB, LANES), jnp.bfloat16),
            pltpu.VMEM(lat.shape, jnp.bfloat16),
        ]
        + [dma((members,))] * 2
        + [dma((count_x,))] * 2
        + [dma((members,))] * 2
        + [dma((members,))] * 2
        + [dma((count_x,))] * 2
        + [dma((members,))] * 2,
        compiler_params=pltpu.CompilerParams(
            collective_id=0, has_side_effects=True, vmem_limit_bytes=48 * 1024 * 1024
        ),
    )(lat, weight, *tables)


def final_kernel(branch_ref, lat_ref, skip_ref, out_ref):
    members, rows, _ = branch_ref.shape
    count = rows // SUB
    branch = [branch_ref[p].astype(jnp.float32) for p in range(members)]
    latent = [lat_ref[p].astype(jnp.float32) for p in range(members)]
    pick = lambda parts, x: jnp.concatenate([a[SUB * x : SUB * (x + 1)] for a in parts], axis=0)
    wide = jnp.concatenate([pick(latent, x) for x in range(count)], axis=1).astype(jnp.bfloat16)
    skip = jnp.dot(skip_ref[...], wide, preferred_element_type=jnp.float32)
    for x in range(count):
        v = pick(branch, x) + skip[:, LANES * x : LANES * (x + 1)]
        inner = v * (0.7978845608028654 + 0.035677408136300125 * (v * v))
        half = 0.5 * v
        out_ref[x, 0] = (half + half * jnp.tanh(inner)).T


def finish(branch, lat, skip_weight, cells_x):
    members, piece_rows, _ = lat.shape
    channels = skip_weight.shape[0]
    rows = cells_x * SUB
    piece = pl.BlockSpec((members, rows, LANES), lambda i: (0, i, 0))
    return pl.pallas_call(
        final_kernel,
        grid=(piece_rows // rows,),
        out_shape=jax.ShapeDtypeStruct((cells_x, piece_rows // rows, LANES, channels), jnp.float32),
        in_specs=[piece, piece, pl.BlockSpec(skip_weight.shape, lambda i: (0, 0))],
        out_specs=pl.BlockSpec((cells_x, 1, LANES, channels), lambda i: (0, i, 0, 0)),
    )(branch, lat, skip_weight.T)


def summed_over_axes(values, axes):
    for axis in axes:
        count = lax.axis_size(axis)
        copies = jnp.broadcast_to(values[None], (count,) + values.shape)
        values = jnp.sum(lax.all_to_all(copies, axis, 0, 0, tiled=True), axis=0)
    return values


def exchange(values, axis, split_axis, concat_axis):
    return lax.all_to_all(
        values.astype(jnp.bfloat16), axis, split_axis=split_axis, concat_axis=concat_axis, tiled=True
    ).astype(jnp.float32)


def body(point_data, neighbours, counts, kernel_in, kernel_mid, kernel_out, spectral, skip_weight):
    count_y = lax.axis_size("gy")
    count_z = lax.axis_size("gz")
    place_x = lax.axis_index("gx")
    place_y = lax.axis_index("gy")
    place_z = lax.axis_index("gz")
    geometry_count, cells_x, cells_y, cells_z = neighbours.shape[0:4]
    per_device = point_data.shape[2]
    channels = skip_weight.shape[0]
    cells = point_data[:, :, None, None, None]
    for dim, axis in enumerate(("gx", "gy", "gz")):
        cells = beside(cells, axis, dim + 2)
    table = cells.reshape(geometry_count, point_data.shape[1], -1)
    owner = neighbours // per_device
    offset_z, width_z = offset(owner % count_z, "gz")
    offset_y, width_y = offset(owner // count_z % count_y, "gy")
    offset_x, _ = offset(owner // (count_z * count_y), "gx")
    block_index = (offset_x * width_y + offset_y) * width_z + offset_z
    slot_index = neighbours % per_device
    centre_y = (
        (place_y * cells_y + jnp.arange(cells_y, dtype=jnp.int32)).astype(jnp.float32) + 0.5
    ) / GRID
    centre_z = (
        (place_z * cells_z + jnp.arange(cells_z, dtype=jnp.int32)).astype(jnp.float32) + 0.5
    ) / GRID
    centre_x = (
        (place_x * cells_x + jnp.arange(cells_x, dtype=jnp.int32)).astype(jnp.float32) + 0.5
    ) / GRID
    shape = (cells_x, cells_y, cells_z)
    rows_y = LANES // cells_z
    node_order = lambda values: jnp.swapaxes(
        values.reshape(values.shape[:-3] + (cells_x, cells_y // rows_y, LANES)), -3, -2
    ).reshape(values.shape[:-3] + (-1, LANES))
    centres = jnp.stack(
        [
            jnp.broadcast_to(centre_x[:, None, None], shape),
            jnp.broadcast_to(centre_y[None, :, None], shape),
            jnp.broadcast_to(centre_z[None, None, :], shape),
        ]
    )
    centres = node_order(centres / SCALE)
    code = block_index * per_device + slot_index
    grouped = (
        count_y * count_z * SUB == channels
        and cells_x * SUB == LANES
        and count_z * MODES // 2 == MODES
        and 2 * (MODES // lax.axis_size("gx")) * MODES == LANES
    )
    latent = []
    for geometry in range(geometry_count):
        turned = node_order(jnp.moveaxis(code[geometry], -1, 0))
        latent.append(
            encode(
                turned,
                node_order(counts[geometry]),
                centres,
                pack_table(table[geometry]),
                kernel_in,
                kernel_mid,
                kernel_out,
                grouped,
            )
        )
    if grouped:
        results = [
            finish(spectral_branch(lat, spectral), lat, skip_weight, cells_x) for lat in latent
        ]
        return jnp.stack(results).reshape(geometry_count, cells_x, cells_y, cells_z, channels)
    latent = jnp.swapaxes(jnp.stack(latent), 2, 3).astype(jnp.bfloat16)
    latent = latent.reshape(geometry_count, cells_y // rows_y, cells_x, LANES, channels)
    latent = jnp.swapaxes(latent, 1, 2)
    latent = latent.reshape(geometry_count, cells_x, cells_y, cells_z, channels)
    cos_centred, sin_centred = tables(GRID, MODES, True)
    cos_third, sin_third = tables(GRID, MODES, False)
    back_cos, back_sin = third_weights(cos_third, sin_third, GRID)
    depth_full = lax.all_to_all(latent, "gz", split_axis=4, concat_axis=3, tiled=True)
    real_part, imag_part = forward_real(
        depth_full.astype(jnp.float32), cos_third, sin_third, "gxyzc,kz->gxykc"
    )
    real_part, imag_part = (
        lax.all_to_all(real_part, "gy", split_axis=3, concat_axis=2, tiled=True),
        lax.all_to_all(imag_part, "gy", split_axis=3, concat_axis=2, tiled=True),
    )
    real_part, imag_part = forward_complex(
        real_part, imag_part, cos_centred, sin_centred, "gxykc,jy->gxjkc"
    )
    real_part, imag_part = (
        lax.all_to_all(real_part, "gx", split_axis=2, concat_axis=1, tiled=True),
        lax.all_to_all(imag_part, "gx", split_axis=2, concat_axis=1, tiled=True),
    )
    real_part, imag_part = forward_complex(
        real_part, imag_part, cos_centred, sin_centred, "gxjkc,ix->gijkc"
    )
    spec_real, spec_imag = (
        exchange(real_part, "gz", split_axis=1, concat_axis=4),
        exchange(imag_part, "gz", split_axis=1, concat_axis=4),
    )
    spec_real = spec_real.astype(jnp.bfloat16)
    spec_imag = spec_imag.astype(jnp.bfloat16)
    mixed_real = jnp.einsum(
        "gijkc,ijkco->gijko", spec_real, spectral[0], preferred_element_type=jnp.float32
    ) - jnp.einsum("gijkc,ijkco->gijko", spec_imag, spectral[1], preferred_element_type=jnp.float32)
    mixed_imag = jnp.einsum(
        "gijkc,ijkco->gijko", spec_real, spectral[1], preferred_element_type=jnp.float32
    ) + jnp.einsum("gijkc,ijkco->gijko", spec_imag, spectral[0], preferred_element_type=jnp.float32)
    first_place = (place_x + place_y + place_z) == 0
    modes = mixed_real.shape[1:4]
    order = sum(lax.broadcasted_iota(jnp.int32, modes, d) for d in range(3))
    zero_mode = ((order == 0) & first_place)[None, ..., None]
    mixed_real = jnp.where(zero_mode, 0.0, mixed_real)
    mixed_imag = jnp.where(zero_mode, 0.0, mixed_imag)
    mixed_real = mixed_real.astype(jnp.bfloat16)
    mixed_imag = mixed_imag.astype(jnp.bfloat16)
    real_part, imag_part = (
        exchange(mixed_real, "gz", split_axis=4, concat_axis=1),
        exchange(mixed_imag, "gz", split_axis=4, concat_axis=1),
    )
    real_part, imag_part = inverse_complex(
        real_part.astype(jnp.float32),
        imag_part.astype(jnp.float32),
        cos_centred,
        sin_centred,
        "gijkc,ix->gxjkc",
    )
    real_part, imag_part = (
        exchange(real_part, "gx", split_axis=1, concat_axis=2),
        exchange(imag_part, "gx", split_axis=1, concat_axis=2),
    )
    real_part, imag_part = inverse_complex(
        real_part, imag_part, cos_centred, sin_centred, "gxjkc,jy->gxykc"
    )
    real_part, imag_part = (
        exchange(real_part, "gy", split_axis=2, concat_axis=3),
        exchange(imag_part, "gy", split_axis=2, concat_axis=3),
    )
    depth_part = inverse_real(real_part, imag_part, back_cos, back_sin, "gxykc,kz->gxyzc")
    branch = exchange(depth_part, "gz", split_axis=3, concat_axis=4)
    skip = jnp.einsum("gxyzc,co->gxyzo", latent, skip_weight, preferred_element_type=jnp.float32)
    cells_total = float(GRID**3)
    variance = (
        summed_over_axes(jnp.sum(branch * branch, axis=(1, 2, 3)), ("gz", "gy", "gx")) / cells_total
    )
    normed = branch / jnp.sqrt(variance + NORM_FLOOR)[:, None, None, None, :]
    return jax.nn.gelu(normed + skip, approximate=True)


def solution(mesh):
    in_specs = (
        P(None, None, ("gx", "gy", "gz")),
        P(None, "gx", "gy", "gz", None),
        P(None, "gx", "gy", "gz"),
        P(),
        P(),
        P(),
        P(None, "gz", "gx", "gy", None, None),
        P(),
    )
    out_specs = P(None, "gx", "gy", "gz", None)
    return jax.shard_map(body, mesh=mesh, in_specs=in_specs, out_specs=out_specs, check_vma=False)
```

```python
import functools
import math

import jax
import jax.numpy as jnp
import numpy as np
from jax import lax
from jax.experimental import pallas as pl
from jax.experimental.pallas import tpu as pltpu
from jax.sharding import PartitionSpec as P

GRID = 64
MODES = 16
NB = 32


HIGH = lax.Precision.HIGH
NORM_FLOOR = 1.0


def tables(length, keep_count, centred):
    position = jnp.arange(length, dtype=jnp.int32)
    frequency = jnp.arange(keep_count, dtype=jnp.int32)
    if centred:
        frequency = jnp.where(
            frequency < keep_count // 2, frequency, frequency + length - keep_count
        )
    phases = frequency[:, None] * position[None, :] % length
    angles = phases.astype(jnp.float32) * (2.0 * math.pi / length)
    return (jnp.cos(angles), jnp.sin(angles))


def third_weights(cos_table, sin_table, length):
    factor = (
        jnp.where(jnp.arange(cos_table.shape[0]) == 0, 1.0, 2.0).astype(jnp.float32)[:, None]
        / length**3
    )
    return (cos_table * factor, sin_table * factor)


def contract(pattern, operand, table):
    return jnp.einsum(pattern, operand, table, precision=HIGH)


def forward_real(values, cos_table, sin_table, pattern):
    return (contract(pattern, values, cos_table), -contract(pattern, values, sin_table))


def forward_complex(real_part, imag_part, cos_table, sin_table, pattern):
    new_real = contract(pattern, real_part, cos_table) + contract(pattern, imag_part, sin_table)
    new_imag = contract(pattern, imag_part, cos_table) - contract(pattern, real_part, sin_table)
    return (new_real, new_imag)


def inverse_complex(real_part, imag_part, cos_table, sin_table, pattern):
    new_real = contract(pattern, real_part, cos_table) - contract(pattern, imag_part, sin_table)
    new_imag = contract(pattern, real_part, sin_table) + contract(pattern, imag_part, cos_table)
    return (new_real, new_imag)


def inverse_real(real_part, imag_part, cos_table, sin_table, pattern):
    return contract(pattern, real_part, cos_table) - contract(pattern, imag_part, sin_table)


SUB = 8
LANES = 128
SCALE = 0.035677408136300125 ** (-1.0 / 3.0)
SHIFT = 0.7978845608028654 * SCALE
FINE = 1023.0
COARSE = 511.0


def double_gelu(y):
    return y + y * jnp.tanh(y * (y * y + jnp.asarray(SHIFT, y.dtype)))


def pick(leaf, bits, low, high, level):
    if high - low == 1:
        return leaf(low)
    half = 1 << (level - 1)
    if low + half >= high:
        return pick(leaf, bits, low, high, level - 1)
    first = pick(leaf, bits, low, low + half, level - 1)
    second = pick(leaf, bits, low + half, high, level - 1)
    return jnp.where(bits[level - 1], second, first)


def over(values, count):
    return values >> (count.bit_length() - 1) if count & (count - 1) == 0 else values // count


def within(values, count):
    return values & (count - 1) if count & (count - 1) == 0 else lax.rem(values, count)


def offset(owner, place, count):
    return within(owner - place + (count + (1 if count > 2 else 0)), count)


def encoder_kernel(
    sizes, grouped, neighbours_ref, counts_ref, table_ref, in_ref, mid_ref, last_ref, out_ref,
    codes, first, middle, final, stack, one, two, total,
):
    count_x, count_y, count_z, per_device = sizes
    place_x, place_y, place_z = lax.axis_index("gx"), lax.axis_index("gy"), lax.axis_index("gz")
    cells_x, cells_y, cells_z, slots = neighbours_ref.shape
    rows_y = LANES // cells_z
    rows = counts_ref.shape[0]
    units = mid_ref.shape[0]
    channels = last_ref.shape[1]
    words, table_rows = in_ref.shape[0] // 3, table_ref.shape[0]
    depth = max(1, (table_rows - 1).bit_length())
    per = stack.shape[0]
    block = total.shape[2] // LANES
    groups = block // SUB
    turns = slots // per
    blocks = rows // block

    iota = lambda shape, d: lax.broadcasted_iota(jnp.int32, shape, d)
    spread = jnp.where(iota((SUB * units, units), 0) % units == iota((SUB * units, units), 1), 1.0, 0.0)
    values = 3 * words
    wide = jnp.where(iota((values, values * SUB), 0) == iota((values, values * SUB), 1) // SUB, 1.0, 0.0)
    narrow = lambda a: a.astype(jnp.bfloat16)
    inputs = in_ref[...].astype(jnp.float32).T
    tiled = jnp.dot(narrow(inputs), narrow(wide), preferred_element_type=jnp.float32)
    tiled = jnp.dot(narrow(spread), narrow(tiled), preferred_element_type=jnp.float32)
    shape = (SUB * units, values * SUB)
    first[...] = narrow(jnp.where(iota(shape, 0) // units == iota(shape, 1) % SUB, tiled, 0.0))
    middle[...] = narrow(mid_ref[...].astype(jnp.float32).T * 0.5)
    turned = narrow(last_ref[...].astype(jnp.float32).T * 0.5)
    for k in range(per):
        final[:, units * k : units * (k + 1)] = turned
    one[...] = jnp.zeros_like(one)
    two[...] = jnp.zeros_like(two)
    total[...] = jnp.zeros_like(total)
    width_y, width_z = min(count_y, 3), min(count_z, 3)

    def prepare(row, carry):
        strip, x = row // cells_x, lax.rem(row, cells_x)
        near = neighbours_ref[x, pl.ds(strip * rows_y, rows_y)].reshape(LANES, slots).T
        owner = over(near, per_device)
        at_z = offset(within(owner, count_z), place_z, count_z)
        at_y = offset(within(over(owner, count_z), count_y), place_y, count_y)
        at_x = offset(over(owner, count_z * count_y), place_x, count_x)
        code = ((at_x * width_y + at_y) * width_z + at_z) * per_device + within(near, per_device)
        codes[pl.ds(pl.multiple_of(row * slots, SUB), slots), :] = code
        return carry

    lax.fori_loop(0, rows, prepare, 0, unroll=min(8, rows))
    lane_ids = iota((SUB, LANES), 1)
    sub_ids = iota((SUB, LANES), 0)
    centre = lambda cell: (cell.astype(jnp.float32) + 0.5) * (1.0 / (GRID * SCALE))
    centre_z = centre(place_z * cells_z + within(lane_ids, cells_z))
    centre_x = [
        centre(place_x * cells_x + within(SUB * g + sub_ids, cells_x)) for g in range(groups)
    ]
    lane_y = over(lane_ids, cells_z) + place_y * cells_y

    def pairs(t):
        here = jnp.minimum(t // turns, blocks - 1)
        turn = lax.rem(t, turns)
        limit = jnp.where(t < blocks * turns, 0, slots)
        centre_y = centre(lane_y + (here * block // cells_x) * rows_y)
        for k in range(per):
            slot = turn * per + k
            for g in range(groups):
                base = here * block + SUB * g
                code = codes[pl.ds(base * slots + slot, SUB, stride=slots), :]
                lane = code & (LANES - 1)
                bits = [(code & (LANES << b)) != 0 for b in range(depth)]
                live = slot + limit < counts_ref[pl.ds(pl.multiple_of(base, SUB), SUB), :]
                found = []
                for w in range(words):
                    leaf = lambda r: jnp.take_along_axis(
                        jnp.broadcast_to(table_ref[r, 3 * w : 3 * w + 1, :], (SUB, LANES)),
                        lane,
                        axis=1,
                        mode="promise_in_bounds",
                    )
                    word = pick(leaf, bits, 0, table_rows, depth)
                    found += [word >> 21, ((word >> 10) & 2047) - 1024, (word & 1023) - 512]
                parts = []
                for v, x in enumerate(found):
                    x = x.astype(jnp.float32) * (1.0 / (SCALE * (COARSE if v % 3 == 2 else FINE)))
                    if v < 3:
                        x = x - (centre_x[g], centre_y, centre_z)[v]
                    parts.append(jnp.where(live, x, 0.0))
                stack[k, :, LANES * g : LANES * (g + 1)] = narrow(jnp.concatenate(parts, axis=0))

    def step(t, carry):
        there = jnp.maximum(t - 2, 0) // turns
        total[there] += jnp.dot(final[...], two[...], preferred_element_type=jnp.float32)
        for k in range(per):
            z = jnp.dot(middle[...], one[k], preferred_element_type=jnp.float32)
            two[units * k : units * (k + 1), :] = double_gelu(narrow(z))
        for k in range(per):
            z = jnp.dot(first[...], stack[k], preferred_element_type=jnp.float32)
            h = double_gelu(narrow(z))
            for r in range(SUB):
                at = r * groups * LANES
                one[k, :, at : at + groups * LANES] = h[units * r : units * (r + 1)]
        pairs(t + 1)
        return carry

    pairs(0)
    lax.fori_loop(0, blocks * turns + 2, step, 0)

    def close(b, carry):
        done = {}
        for r in range(SUB):
            for g in range(groups):
                at = (r * groups + g) * LANES
                row = SUB * g + r
                count = counts_ref[pl.ds(b * block + row, 1), :].astype(jnp.float32)
                done[row] = total[b, :, at : at + LANES] * (SCALE / count)
                if not grouped:
                    out_ref[b * block + row] = done[row]
        if grouped:
            for q in range(channels // SUB):
                out_ref[q, pl.ds(pl.multiple_of(b * block * SUB, SUB * SUB), block * SUB), :] = narrow(
                    jnp.concatenate(
                        [done[row][SUB * q : SUB * (q + 1)] for row in range(block)], axis=0
                    )
                )
        return carry

    lax.fori_loop(0, blocks, close, 0)


def encode(neighbours, counts, table, kernel_in, kernel_mid, kernel_out, per_device, grouped):
    rows = counts.shape[0]
    slots = neighbours.shape[-1]
    units, channels = kernel_out.shape
    block = min(2 * SUB, rows)
    per = 2
    if grouped:
        shape = jax.ShapeDtypeStruct((channels // SUB, rows * SUB, LANES), jnp.bfloat16)
    else:
        shape = jax.ShapeDtypeStruct((rows, channels, LANES), jnp.float32)
    sizes = tuple(lax.axis_size(a) for a in ("gx", "gy", "gz")) + (per_device,)
    vmem = lambda: pl.BlockSpec(memory_space=pltpu.VMEM)
    values = kernel_in.shape[0]
    return pl.pallas_call(
        functools.partial(encoder_kernel, sizes, grouped),
        out_shape=shape,
        in_specs=[vmem() for _ in range(6)],
        out_specs=vmem(),
        scratch_shapes=[
            pltpu.VMEM((rows * slots, LANES), jnp.int32),
            pltpu.VMEM((SUB * units, values * SUB), jnp.bfloat16),
            pltpu.VMEM((units, units), jnp.bfloat16),
            pltpu.VMEM((channels, per * units), jnp.bfloat16),
            pltpu.VMEM((per, values * SUB, block // SUB * LANES), jnp.bfloat16),
            pltpu.VMEM((per, units, block * LANES), jnp.bfloat16),
            pltpu.VMEM((per * units, block * LANES), jnp.bfloat16),
            pltpu.VMEM((rows // block, channels, block * LANES), jnp.float32),
        ],
        compiler_params=pltpu.CompilerParams(vmem_limit_bytes=40 * 1024 * 1024),
    )(neighbours, counts, table, kernel_in, kernel_mid, kernel_out)


def halo_kernel(sizes, points_ref, out_ref, near, send, recv):
    places = [lax.axis_index(a) for a in ("gx", "gy", "gz")]
    widths = [min(n, 3) for n in sizes]
    home = [1 if n > 2 else 0 for n in sizes]
    blocks = [
        (x, y, z) for x in range(widths[0]) for y in range(widths[1]) for z in range(widths[2])
    ]
    number = lambda b: (b[0] * widths[1] + b[1]) * widths[2] + b[2]

    def reader(block):
        there = [lax.rem(p - o + h + n, n) for p, o, h, n in zip(places, block, home, sizes)]
        return dict(zip(("gx", "gy", "gz"), there))

    others = [b for b in blocks if list(b) != home]
    barrier = pltpu.get_barrier_semaphore()
    for block in others:
        pl.semaphore_signal(
            barrier, inc=1, device_id=reader(block), device_id_type=pl.DeviceIdType.MESH
        )
    pl.semaphore_wait(barrier, len(others))
    copies = {}
    for block in others:
        b = number(block)
        copies[b] = pltpu.make_async_remote_copy(
            src_ref=points_ref,
            dst_ref=near.at[b],
            send_sem=send.at[b],
            recv_sem=recv.at[b],
            device_id=reader(block),
            device_id_type=pl.DeviceIdType.MESH,
        )
        copies[b].start()
    pieces = points_ref.shape[1] // LANES
    for block in [tuple(home)] + others:
        b = number(block)
        if b in copies:
            copies[b].wait()
            values = near[b]
        else:
            values = points_ref[...]
        values = jnp.concatenate([values, values[0 : SUB - values.shape[0]]], axis=0)
        fine = jnp.round(values * FINE).astype(jnp.int32)
        coarse = jnp.round(values * COARSE).astype(jnp.int32)
        for r in range(pieces):
            part = fine[:, LANES * r : LANES * (r + 1)]
            third = coarse[:, LANES * r : LANES * (r + 1)]
            out_ref[b * pieces + r] = (
                part * 2097152
                + (pltpu.roll(part, SUB - 1, 0) + 1024) * 1024
                + (pltpu.roll(third, SUB - 2, 0) + 512)
            )


def point_table(points):
    sizes = tuple(lax.axis_size(a) for a in ("gx", "gy", "gz"))
    blocks = math.prod(min(n, 3) for n in sizes)
    vmem = pl.BlockSpec(memory_space=pltpu.VMEM)
    return pl.pallas_call(
        functools.partial(halo_kernel, sizes),
        out_shape=jax.ShapeDtypeStruct((blocks * points.shape[1] // LANES, SUB, LANES), jnp.int32),
        in_specs=[vmem],
        out_specs=vmem,
        scratch_shapes=[
            pltpu.VMEM((blocks,) + points.shape, jnp.float32),
            pltpu.SemaphoreType.DMA((blocks,)),
            pltpu.SemaphoreType.DMA((blocks,)),
        ],
        compiler_params=pltpu.CompilerParams(collective_id=1, has_side_effects=True),
    )(points)


def lane_maps(quarters, parts, inner_k, inner_j):
    grid = np.indices((quarters, 2, parts, inner_k, inner_j)).reshape(5, -1)
    return grid[0] * inner_j + grid[4], grid[2] * inner_k + grid[3], grid[1]


def spectral_tables(count_x, count_y, count_z, cells_x, cells_y, cells_z, group):
    keep = MODES
    signed = np.where(np.arange(keep) < keep // 2, np.arange(keep), np.arange(keep) - keep)
    mode_j, mode_k, imaginary = lane_maps(count_x, count_y, keep // count_y, keep // count_x)
    turn = 2.0 * np.pi / GRID
    rows_y = LANES // cells_z
    place_z, row_y, cell_z = np.indices((count_z, rows_y, cells_z)).reshape(3, -1)
    phase = turn * (
        (signed[mode_j] * row_y[:, None] + mode_k * (place_z * cells_z + cell_z)[:, None]) % GRID
    )
    forward = np.where(imaginary, -np.sin(phase), np.cos(phase))
    weight = np.where(mode_k == 0, 1.0, 2.0)
    inverse = (np.where(imaginary, -np.sin(phase), np.cos(phase)) * weight).T
    sign = np.where(imaginary, -1.0, 1.0)
    strip = turn * ((signed[mode_j] * (rows_y * np.arange(GRID // rows_y))[:, None]) % GRID)
    strips = np.stack([np.cos(strip), np.sin(strip) * sign])
    cell = np.arange(count_x * cells_x).reshape(count_x, 1, cells_x)
    angle = turn * ((signed[:, None] * cell) % GRID)
    eye = np.eye(group)

    def expand(values):
        wide = np.einsum("pab,cd->pacbd", values, eye)
        return wide.reshape(count_x, values.shape[1] * group, values.shape[2] * group)

    ahead = np.concatenate([expand(np.cos(angle)), expand(np.sin(angle))], axis=2)
    back = np.swapaxes(angle, 1, 2)
    back = np.concatenate([expand(np.cos(back)), expand(np.sin(back))], axis=2)
    partner = (keep - mode_j) % keep
    same = (
        (mode_j[:, None] == partner[None, :])
        & (mode_k[:, None] == 0)
        & (mode_k[None, :] == 0)
        & (imaginary[:, None] == imaginary[None, :])
        & (mode_j[:, None] != keep // 2)
    )
    flip = same * sign[None, :]
    power = np.where(mode_k == 0, 0.5, 2.0)
    lanes = np.stack([sign, power])
    narrow = lambda array: jnp.asarray(array.astype(np.float32), jnp.bfloat16)
    single = lambda array: jnp.asarray(array.astype(np.float32))
    return (
        narrow(forward),
        narrow(inverse),
        single(strips),
        narrow(ahead),
        narrow(back),
        narrow(flip),
        single(lanes),
    )


def swap_halves(values):
    return jnp.concatenate(
        [
            pltpu.roll(values[:, at : at + LANES], LANES // 2, 1)
            for at in range(0, values.shape[1], LANES)
        ],
        axis=1,
    )


def split(values):
    upper = values.astype(jnp.bfloat16)
    return upper, (values - upper.astype(jnp.float32)).astype(jnp.bfloat16)


def spectral_kernel(
    count_x,
    count_y,
    count_z,
    lat_ref,
    weight_ref,
    forward_ref,
    inverse_ref,
    strips_ref,
    ahead_ref,
    back_ref,
    flip_ref,
    lanes_ref,
    out_ref,
    came,
    plane,
    sums,
    sums_in,
    own,
    own_in,
    turned,
    mixed,
    mixed_in,
    joined,
    all_modes,
    pieces,
    send_a, recv_a, send_b, recv_b, send_c, recv_c, send_d, recv_d, send_e, recv_e, send_f, recv_f,
):
    place_x, place_y, place_z = lax.axis_index("gx"), lax.axis_index("gy"), lax.axis_index("gz")
    members = count_y * count_z
    me = place_y * count_z + place_z
    group = SUB
    strip_rows = plane.shape[0]
    half_modes = MODES // count_z
    inner = (MODES // count_x) * (MODES // count_y)
    mesh_id = pl.DeviceIdType.MESH

    def member(t):
        other = lax.rem(me + t, members)
        return other, {"gy": other // count_z, "gz": lax.rem(other, count_z)}

    def column(t):
        other = lax.rem(place_x + t, count_x)
        return other, {"gx": other}

    barrier = pltpu.get_barrier_semaphore()
    for t in range(1, members):
        pl.semaphore_signal(barrier, inc=1, device_id=member(t)[1], device_id_type=mesh_id)
    for t in range(1, count_x):
        pl.semaphore_signal(barrier, inc=1, device_id=column(t)[1], device_id_type=mesh_id)
    pl.semaphore_wait(barrier, members - 1 + count_x - 1)

    def exchange_with(peer, total, source, target, send, recv):
        copies = []
        for t in range(1, total):
            other, device = peer(t)
            copy = pltpu.make_async_remote_copy(
                src_ref=source(other),
                dst_ref=target,
                send_sem=send.at[t],
                recv_sem=recv.at[t],
                device_id=device,
                device_id_type=mesh_id,
            )
            copy.start()
            copies.append(copy)
        return copies

    def apart(d, e):
        other = {
            "gy": lax.rem(place_y + count_y - d, count_y),
            "gz": lax.rem(place_z + e, count_z),
        }
        return other["gy"] * count_z + other["gz"], other

    def send_to(d, e, source, target, send, recv):
        other, device = apart(d, e)
        copy = pltpu.make_async_remote_copy(
            src_ref=source.at[other],
            dst_ref=target.at[me],
            send_sem=send.at[d * count_z + e],
            recv_sem=recv.at[d * count_z + e],
            device_id=device,
            device_id_type=mesh_id,
        )
        copy.start()
        return copy

    steps = [(d, e) for d in range(count_y) for e in range(count_z)]
    arrivals = {s: send_to(*s, lat_ref, came, send_a, recv_a) for s in steps if s != (0, 0)}
    came[me] = lat_ref[me]
    sign = lanes_ref[0:1, :]
    plane[...] = jnp.zeros_like(plane)
    chunks = came.shape[1] // strip_rows

    def ahead_step(source, chunk, carry):
        strip = source * chunks + chunk
        at = pl.multiple_of(chunk * strip_rows, strip_rows)
        block = jnp.concatenate(
            [came[source * count_z + z, pl.ds(at, strip_rows), :] for z in range(count_z)], axis=1
        )
        part = jnp.dot(block, forward_ref[...], preferred_element_type=jnp.float32)
        cosine = strips_ref[0, pl.ds(strip, 1), :]
        sine = strips_ref[1, pl.ds(strip, 1), :]
        plane[...] += part * cosine + swap_halves(part) * sine
        return carry

    for d in range(count_y):
        for e in range(count_z):
            if (d, e) in arrivals:
                arrivals[d, e].wait()
        source = lax.rem(place_y + d, count_y)
        lax.fori_loop(0, chunks, functools.partial(ahead_step, source), 0)
    whole = plane[...]
    whole_high, whole_low = split(whole)
    turn_high, turn_low = split(swap_halves(whole) * sign)
    table = ahead_ref[place_x]
    total = jnp.dot(
        table, jnp.concatenate([whole_high, turn_high], axis=0), preferred_element_type=jnp.float32
    ) + jnp.dot(
        table, jnp.concatenate([whole_low, turn_low], axis=0), preferred_element_type=jnp.float32
    )
    for q in range(count_x):
        sums[q] = total[:, LANES * q : LANES * (q + 1)]
    copies = exchange_with(column, count_x, lambda p: sums.at[p], sums_in.at[place_x], send_b, recv_b)
    sums_in[place_x] = sums[place_x]
    for copy in copies:
        copy.wait()
    spectrum = sums_in[0]
    for q in range(1, count_x):
        spectrum = spectrum + sums_in[q]
    half_rows = half_modes * group
    for z in range(count_z):
        own[z] = spectrum[half_rows * z : half_rows * (z + 1)].astype(jnp.bfloat16)

    copies = exchange_with(
        member, members, lambda p: own.at[lax.rem(p, count_z)], own_in.at[me], send_c, recv_c
    )
    own_in[me] = own[place_z]
    mixed_rows = lax.broadcasted_iota(jnp.int32, (2 * inner, LANES), 0) % inner
    mixed_lanes = lax.broadcasted_iota(jnp.int32, (2 * inner, LANES), 1) // (LANES // 2)
    modes_j = MODES // count_x
    modes_k = MODES // count_y
    row_mode = (mixed_rows % modes_j) * modes_k + mixed_rows // modes_j
    first_place = (place_x + place_y + place_z) == 0
    mode_zero = lax.broadcasted_iota(jnp.int32, (inner, LANES // 2), 0) == 0
    turned[...] = jnp.zeros_like(turned)
    for copy in copies:
        copy.wait()
    arrived = [own_in[p].astype(jnp.float32) for p in range(members)]
    for i in range(half_modes):
        column_values = jnp.concatenate([a[group * i : group * (i + 1)] for a in arrived], axis=0)
        column_values = jnp.concatenate([column_values, column_values], axis=0)
        mixed[i] = column_values.T
        at = pl.multiple_of(place_y * inner, inner)
        both = jnp.concatenate(
            [mixed[i, pl.ds(at, inner), :], mixed[i, pl.ds(LANES // 2 + at, inner), :]], axis=0
        )
        wide = jnp.concatenate(
            [
                jnp.where(row_mode == 2 * t + mixed_lanes, both, 0.0).astype(jnp.bfloat16)
                for t in range(inner // 2)
            ],
            axis=1,
        )
        by_real = jnp.dot(wide, weight_ref[0, i], preferred_element_type=jnp.float32)
        by_imag = jnp.dot(wide, weight_ref[1, i], preferred_element_type=jnp.float32)
        real = by_real[:inner] - by_imag[inner:]
        imag = by_imag[:inner] + by_real[inner:]
        if i == 0:
            drop = jnp.logical_and(mode_zero, first_place)
            real = jnp.where(drop, 0.0, real)
            imag = jnp.where(drop, 0.0, imag)
        turned[i, pl.ds(at, inner), 0 : LANES // 2] = real
        turned[i, pl.ds(LANES // 2 + at, inner), 0 : LANES // 2] = imag
    flat = [turned[i].T for i in range(half_modes)]
    for p in range(members):
        joined[p] = jnp.concatenate(
            [f[group * p : group * (p + 1)] for f in flat], axis=0
        ).astype(jnp.bfloat16)

    copies = exchange_with(member, members, lambda p: joined.at[p], mixed_in.at[me], send_d, recv_d)
    mixed_in[me] = joined[me]
    for copy in copies:
        copy.wait()
    parts = []
    for z in range(count_z):
        value = mixed_in[z].astype(jnp.float32)
        for y in range(1, count_y):
            value = value + mixed_in[y * count_z + z].astype(jnp.float32)
        parts.append(value)
    all_modes[place_x] = jnp.concatenate(parts, axis=0).astype(jnp.bfloat16)
    copies = exchange_with(
        column, count_x, lambda p: all_modes.at[place_x], all_modes.at[place_x], send_e, recv_e
    )
    for copy in copies:
        copy.wait()
    modes = jnp.concatenate([all_modes[q] for q in range(count_x)], axis=1)
    scaled = modes.astype(jnp.float32) * (1.0 / GRID**3)
    partner = jnp.dot(modes, flip_ref[...], preferred_element_type=jnp.float32) * (1.0 / GRID**3)
    energy = None
    for i in range(MODES):
        value = scaled[group * i : group * (i + 1)]
        term = value * value * lanes_ref[1:2, :]
        if i != MODES // 2:
            other = (MODES - i) % MODES
            term = term + 0.5 * value * partner[group * other : group * (other + 1)]
        energy = term if energy is None else energy + term
    variance = jnp.sum(energy, axis=1, keepdims=True)
    gain = 1.0 / jnp.sqrt(variance + NORM_FLOOR)
    rotated = (swap_halves(scaled * float(GRID**3)) * -sign).astype(jnp.bfloat16)
    back = jnp.dot(
        back_ref[place_x], jnp.concatenate([modes, rotated], axis=0), preferred_element_type=jnp.float32
    )
    back = back.reshape(-1, group, back.shape[1]) * (gain * (1.0 / GRID**3))[None]
    plane[...] = back.reshape(plane.shape)

    def back_step(source, chunk, carry):
        strip = source * chunks + chunk
        at = pl.multiple_of(chunk * strip_rows, strip_rows)
        cosine = strips_ref[0, pl.ds(strip, 1), :]
        sine = strips_ref[1, pl.ds(strip, 1), :]
        value = plane[...]
        value = (value * cosine - swap_halves(value) * sine).astype(jnp.bfloat16)
        result = jnp.dot(value, inverse_ref[...], preferred_element_type=jnp.float32)
        for z in range(count_z):
            pieces[source * count_z + z, pl.ds(at, strip_rows), :] = result[
                :, LANES * z : LANES * (z + 1)
            ].astype(jnp.bfloat16)
        return carry

    copies = []
    for d in [*range(1, count_y), 0]:
        source = lax.rem(place_y + count_y - d, count_y)
        lax.fori_loop(0, chunks, functools.partial(back_step, source), 0)
        copies += [
            send_to(d, e, pieces, out_ref, send_f, recv_f) for e in range(count_z) if (d, e) != (0, 0)
        ]
    out_ref[me] = pieces[me]
    for copy in copies:
        copy.wait()


def spectral_branch(lat, spectral):
    count_x, count_y, count_z = (lax.axis_size(a) for a in ("gx", "gy", "gz"))
    members, piece_rows, _ = lat.shape
    cells_x, cells_y, cells_z = GRID // count_x, GRID // count_y, GRID // count_z
    strip_rows = cells_x * SUB
    half_modes = MODES // count_z
    channels = spectral.shape[-1]
    inner = (MODES // count_x) * (MODES // count_y)
    lanes = 2 * MODES * MODES
    tables = spectral_tables(count_x, count_y, count_z, cells_x, cells_y, cells_z, SUB)
    weight = spectral.reshape(2, half_modes, inner * channels, channels)
    vmem = lambda: pl.BlockSpec(memory_space=pltpu.VMEM)
    half = half_modes * SUB
    dma = pltpu.SemaphoreType.DMA
    return pl.pallas_call(
        functools.partial(spectral_kernel, count_x, count_y, count_z),
        out_shape=jax.ShapeDtypeStruct(lat.shape, jnp.bfloat16),
        in_specs=[vmem() for _ in range(9)],
        out_specs=vmem(),
        scratch_shapes=[
            pltpu.VMEM(lat.shape, jnp.bfloat16),
            pltpu.VMEM((strip_rows, lanes), jnp.float32),
            pltpu.VMEM((count_x, MODES * SUB, LANES), jnp.float32),
            pltpu.VMEM((count_x, MODES * SUB, LANES), jnp.float32),
            pltpu.VMEM((count_z, half, LANES), jnp.bfloat16),
            pltpu.VMEM((members, half, LANES), jnp.bfloat16),
            pltpu.VMEM((half_modes, LANES, LANES), jnp.float32),
            pltpu.VMEM((half_modes, LANES, LANES), jnp.float32),
            pltpu.VMEM((members, half, LANES), jnp.bfloat16),
            pltpu.VMEM((members, half, LANES), jnp.bfloat16),
            pltpu.VMEM((count_x, MODES * SUB, LANES), jnp.bfloat16),
            pltpu.VMEM(lat.shape, jnp.bfloat16),
        ]
        + [dma((members,))] * 2
        + [dma((count_x,))] * 2
        + [dma((members,))] * 2
        + [dma((members,))] * 2
        + [dma((count_x,))] * 2
        + [dma((members,))] * 2,
        compiler_params=pltpu.CompilerParams(
            collective_id=0, has_side_effects=True, vmem_limit_bytes=48 * 1024 * 1024
        ),
    )(lat, weight, *tables)


def final_kernel(branch_ref, lat_ref, skip_ref, out_ref):
    members, rows, _ = branch_ref.shape
    count = rows // SUB
    branch = [branch_ref[p].astype(jnp.float32) for p in range(members)]
    latent = [lat_ref[p].astype(jnp.float32) for p in range(members)]
    pick = lambda parts, x: jnp.concatenate([a[SUB * x : SUB * (x + 1)] for a in parts], axis=0)
    wide = jnp.concatenate([pick(latent, x) for x in range(count)], axis=1).astype(jnp.bfloat16)
    skip = jnp.dot(skip_ref[...], wide, preferred_element_type=jnp.float32)
    for x in range(count):
        v = pick(branch, x) + skip[:, LANES * x : LANES * (x + 1)]
        inner = v * (0.7978845608028654 + 0.035677408136300125 * (v * v))
        half = 0.5 * v
        out_ref[x, 0] = (half + half * jnp.tanh(inner)).T


def finish(branch, lat, skip_weight, cells_x):
    members, piece_rows, _ = lat.shape
    channels = skip_weight.shape[0]
    rows = cells_x * SUB
    piece = pl.BlockSpec((members, rows, LANES), lambda i: (0, i, 0))
    return pl.pallas_call(
        final_kernel,
        grid=(piece_rows // rows,),
        out_shape=jax.ShapeDtypeStruct((cells_x, piece_rows // rows, LANES, channels), jnp.float32),
        in_specs=[piece, piece, pl.BlockSpec(skip_weight.shape, lambda i: (0, 0))],
        out_specs=pl.BlockSpec((cells_x, 1, LANES, channels), lambda i: (0, i, 0, 0)),
    )(branch, lat, skip_weight.T)


def summed_over_axes(values, axes):
    for axis in axes:
        count = lax.axis_size(axis)
        copies = jnp.broadcast_to(values[None], (count,) + values.shape)
        values = jnp.sum(lax.all_to_all(copies, axis, 0, 0, tiled=True), axis=0)
    return values


def exchange(values, axis, split_axis, concat_axis):
    return lax.all_to_all(
        values.astype(jnp.bfloat16), axis, split_axis=split_axis, concat_axis=concat_axis, tiled=True
    ).astype(jnp.float32)


def body(point_data, neighbours, counts, kernel_in, kernel_mid, kernel_out, spectral, skip_weight):
    count_y = lax.axis_size("gy")
    count_z = lax.axis_size("gz")
    place_x = lax.axis_index("gx")
    place_y = lax.axis_index("gy")
    place_z = lax.axis_index("gz")
    geometry_count, cells_x, cells_y, cells_z = neighbours.shape[0:4]
    per_device = point_data.shape[2]
    channels = skip_weight.shape[0]
    rows_y = LANES // cells_z
    node_order = lambda values: jnp.swapaxes(
        values.reshape(cells_x, cells_y // rows_y, LANES), 0, 1
    ).reshape(-1, LANES)
    grouped = (
        count_y * count_z * SUB == channels
        and cells_x * SUB == LANES
        and count_z * MODES // 2 == MODES
        and 2 * (MODES // lax.axis_size("gx")) * MODES == LANES
    )
    latent = []
    for geometry in range(geometry_count):
        latent.append(
            encode(
                neighbours[geometry],
                node_order(counts[geometry]),
                point_table(point_data[geometry]),
                kernel_in,
                kernel_mid,
                kernel_out,
                per_device,
                grouped,
            )
        )
    if grouped:
        results = [
            finish(spectral_branch(lat, spectral), lat, skip_weight, cells_x) for lat in latent
        ]
        return jnp.stack(results).reshape(geometry_count, cells_x, cells_y, cells_z, channels)
    latent = jnp.swapaxes(jnp.stack(latent), 2, 3).astype(jnp.bfloat16)
    latent = latent.reshape(geometry_count, cells_y // rows_y, cells_x, LANES, channels)
    latent = jnp.swapaxes(latent, 1, 2)
    latent = latent.reshape(geometry_count, cells_x, cells_y, cells_z, channels)
    cos_centred, sin_centred = tables(GRID, MODES, True)
    cos_third, sin_third = tables(GRID, MODES, False)
    back_cos, back_sin = third_weights(cos_third, sin_third, GRID)
    depth_full = lax.all_to_all(latent, "gz", split_axis=4, concat_axis=3, tiled=True)
    real_part, imag_part = forward_real(
        depth_full.astype(jnp.float32), cos_third, sin_third, "gxyzc,kz->gxykc"
    )
    real_part, imag_part = (
        lax.all_to_all(real_part, "gy", split_axis=3, concat_axis=2, tiled=True),
        lax.all_to_all(imag_part, "gy", split_axis=3, concat_axis=2, tiled=True),
    )
    real_part, imag_part = forward_complex(
        real_part, imag_part, cos_centred, sin_centred, "gxykc,jy->gxjkc"
    )
    real_part, imag_part = (
        lax.all_to_all(real_part, "gx", split_axis=2, concat_axis=1, tiled=True),
        lax.all_to_all(imag_part, "gx", split_axis=2, concat_axis=1, tiled=True),
    )
    real_part, imag_part = forward_complex(
        real_part, imag_part, cos_centred, sin_centred, "gxjkc,ix->gijkc"
    )
    spec_real, spec_imag = (
        exchange(real_part, "gz", split_axis=1, concat_axis=4),
        exchange(imag_part, "gz", split_axis=1, concat_axis=4),
    )
    spec_real = spec_real.astype(jnp.bfloat16)
    spec_imag = spec_imag.astype(jnp.bfloat16)
    mixed_real = jnp.einsum(
        "gijkc,ijkco->gijko", spec_real, spectral[0], preferred_element_type=jnp.float32
    ) - jnp.einsum("gijkc,ijkco->gijko", spec_imag, spectral[1], preferred_element_type=jnp.float32)
    mixed_imag = jnp.einsum(
        "gijkc,ijkco->gijko", spec_real, spectral[1], preferred_element_type=jnp.float32
    ) + jnp.einsum("gijkc,ijkco->gijko", spec_imag, spectral[0], preferred_element_type=jnp.float32)
    first_place = (place_x + place_y + place_z) == 0
    modes = mixed_real.shape[1:4]
    order = sum(lax.broadcasted_iota(jnp.int32, modes, d) for d in range(3))
    zero_mode = ((order == 0) & first_place)[None, ..., None]
    mixed_real = jnp.where(zero_mode, 0.0, mixed_real)
    mixed_imag = jnp.where(zero_mode, 0.0, mixed_imag)
    mixed_real = mixed_real.astype(jnp.bfloat16)
    mixed_imag = mixed_imag.astype(jnp.bfloat16)
    real_part, imag_part = (
        exchange(mixed_real, "gz", split_axis=4, concat_axis=1),
        exchange(mixed_imag, "gz", split_axis=4, concat_axis=1),
    )
    real_part, imag_part = inverse_complex(
        real_part.astype(jnp.float32),
        imag_part.astype(jnp.float32),
        cos_centred,
        sin_centred,
        "gijkc,ix->gxjkc",
    )
    real_part, imag_part = (
        exchange(real_part, "gx", split_axis=1, concat_axis=2),
        exchange(imag_part, "gx", split_axis=1, concat_axis=2),
    )
    real_part, imag_part = inverse_complex(
        real_part, imag_part, cos_centred, sin_centred, "gxjkc,jy->gxykc"
    )
    real_part, imag_part = (
        exchange(real_part, "gy", split_axis=2, concat_axis=3),
        exchange(imag_part, "gy", split_axis=2, concat_axis=3),
    )
    depth_part = inverse_real(real_part, imag_part, back_cos, back_sin, "gxykc,kz->gxyzc")
    branch = exchange(depth_part, "gz", split_axis=3, concat_axis=4)
    skip = jnp.einsum("gxyzc,co->gxyzo", latent, skip_weight, preferred_element_type=jnp.float32)
    cells_total = float(GRID**3)
    variance = (
        summed_over_axes(jnp.sum(branch * branch, axis=(1, 2, 3)), ("gz", "gy", "gx")) / cells_total
    )
    normed = branch / jnp.sqrt(variance + NORM_FLOOR)[:, None, None, None, :]
    return jax.nn.gelu(normed + skip, approximate=True)


def solution(mesh):
    in_specs = (
        P(None, None, ("gx", "gy", "gz")),
        P(None, "gx", "gy", "gz", None),
        P(None, "gx", "gy", "gz"),
        P(),
        P(),
        P(),
        P(None, "gz", "gx", "gy", None, None),
        P(),
    )
    out_specs = P(None, "gx", "gy", "gz", None)
    return jax.shard_map(body, mesh=mesh, in_specs=in_specs, out_specs=out_specs, check_vma=False)
```

```python
import functools
import math

import jax
import jax.numpy as jnp
import numpy as np
from jax import lax
from jax.experimental import pallas as pl
from jax.experimental.pallas import tpu as pltpu
from jax.sharding import PartitionSpec as P

GRID = 64
MODES = 16
NB = 32


HIGH = lax.Precision.HIGH
NORM_FLOOR = 1.0


def tables(length, keep_count, centred):
    position = jnp.arange(length, dtype=jnp.int32)
    frequency = jnp.arange(keep_count, dtype=jnp.int32)
    if centred:
        frequency = jnp.where(
            frequency < keep_count // 2, frequency, frequency + length - keep_count
        )
    phases = frequency[:, None] * position[None, :] % length
    angles = phases.astype(jnp.float32) * (2.0 * math.pi / length)
    return (jnp.cos(angles), jnp.sin(angles))


def third_weights(cos_table, sin_table, length):
    factor = (
        jnp.where(jnp.arange(cos_table.shape[0]) == 0, 1.0, 2.0).astype(jnp.float32)[:, None]
        / length**3
    )
    return (cos_table * factor, sin_table * factor)


def contract(pattern, operand, table):
    return jnp.einsum(pattern, operand, table, precision=HIGH)


def forward_real(values, cos_table, sin_table, pattern):
    return (contract(pattern, values, cos_table), -contract(pattern, values, sin_table))


def forward_complex(real_part, imag_part, cos_table, sin_table, pattern):
    new_real = contract(pattern, real_part, cos_table) + contract(pattern, imag_part, sin_table)
    new_imag = contract(pattern, imag_part, cos_table) - contract(pattern, real_part, sin_table)
    return (new_real, new_imag)


def inverse_complex(real_part, imag_part, cos_table, sin_table, pattern):
    new_real = contract(pattern, real_part, cos_table) - contract(pattern, imag_part, sin_table)
    new_imag = contract(pattern, real_part, sin_table) + contract(pattern, imag_part, cos_table)
    return (new_real, new_imag)


def inverse_real(real_part, imag_part, cos_table, sin_table, pattern):
    return contract(pattern, real_part, cos_table) - contract(pattern, imag_part, sin_table)


SUB = 8
LANES = 128
SCALE = 0.035677408136300125 ** (-1.0 / 3.0)
SHIFT = 0.7978845608028654 * SCALE
FINE = 1023.0
COARSE = 511.0


def double_gelu(y):
    return y + y * jnp.tanh(y * (y * y + jnp.asarray(SHIFT, y.dtype)))


def pick(leaf, bits, low, high, level):
    if high - low == 1:
        return leaf(low)
    half = 1 << (level - 1)
    if low + half >= high:
        return pick(leaf, bits, low, high, level - 1)
    first = pick(leaf, bits, low, low + half, level - 1)
    second = pick(leaf, bits, low + half, high, level - 1)
    return jnp.where(bits[level - 1], second, first)


def over(values, count):
    return values >> (count.bit_length() - 1) if count & (count - 1) == 0 else values // count


def within(values, count):
    return values & (count - 1) if count & (count - 1) == 0 else lax.rem(values, count)


def offset(owner, place, count):
    return within(owner - place + (count + (1 if count > 2 else 0)), count)


def encoder_kernel(
    cells, grouped, counts_ref, table_ref, codes, first, middle, final, out_ref,
    stack, one, two, total,
):
    place_x, place_y, place_z = lax.axis_index("gx"), lax.axis_index("gy"), lax.axis_index("gz")
    cells_x, cells_y, cells_z = cells
    rows_y = LANES // cells_z
    rows = counts_ref.shape[0]
    slots = codes.shape[0] // rows
    units = middle.shape[0]
    channels = final.shape[0]
    words, table_rows = first.shape[1] // (3 * SUB), table_ref.shape[1]
    depth = max(1, (table_rows - 1).bit_length())
    per = stack.shape[0]
    block = total.shape[2] // LANES
    groups = block // SUB
    turns = slots // per
    blocks = rows // block
    iota = lambda shape, d: lax.broadcasted_iota(jnp.int32, shape, d)
    narrow = lambda a: a.astype(jnp.bfloat16)
    one[...] = jnp.zeros_like(one)
    two[...] = jnp.zeros_like(two)
    total[...] = jnp.zeros_like(total)
    lane_ids = iota((SUB, LANES), 1)
    sub_ids = iota((SUB, LANES), 0)
    centre = lambda cell: (cell.astype(jnp.float32) + 0.5) * (1.0 / (GRID * SCALE))
    centre_z = centre(place_z * cells_z + within(lane_ids, cells_z))
    centre_x = [
        centre(place_x * cells_x + within(SUB * g + sub_ids, cells_x)) for g in range(groups)
    ]
    lane_y = over(lane_ids, cells_z) + place_y * cells_y

    def pairs(t):
        here = jnp.minimum(t // turns, blocks - 1)
        turn = lax.rem(t, turns)
        limit = jnp.where(t < blocks * turns, 0, slots)
        centre_y = centre(lane_y + (here * block // cells_x) * rows_y)
        for k in range(per):
            slot = turn * per + k
            for g in range(groups):
                base = here * block + SUB * g
                code = codes[pl.ds(base * slots + slot, SUB, stride=slots), :]
                lane = code & (LANES - 1)
                bits = [(code & (LANES << b)) != 0 for b in range(depth)]
                live = slot + limit < counts_ref[pl.ds(pl.multiple_of(base, SUB), SUB), :]
                found = []
                for w in range(words):
                    leaf = lambda r: jnp.take_along_axis(
                        jnp.broadcast_to(table_ref[w, r : r + 1, :], (SUB, LANES)),
                        lane,
                        axis=1,
                        mode="promise_in_bounds",
                    )
                    word = pick(leaf, bits, 0, table_rows, depth)
                    found += [word >> 21, ((word >> 10) & 2047) - 1024, (word & 1023) - 512]
                parts = []
                for v, x in enumerate(found):
                    x = x.astype(jnp.float32) * (1.0 / (SCALE * (COARSE if v % 3 == 2 else FINE)))
                    if v < 3:
                        x = x - (centre_x[g], centre_y, centre_z)[v]
                    parts.append(jnp.where(live, x, 0.0))
                stack[k, :, LANES * g : LANES * (g + 1)] = narrow(jnp.concatenate(parts, axis=0))

    def step(t, carry):
        there = jnp.maximum(t - 2, 0) // turns
        total[there] += jnp.dot(final[...], two[...], preferred_element_type=jnp.float32)
        for k in range(per):
            z = jnp.dot(middle[...], one[k], preferred_element_type=jnp.float32)
            two[units * k : units * (k + 1), :] = double_gelu(narrow(z))
        for k in range(per):
            z = jnp.dot(first[...], stack[k], preferred_element_type=jnp.float32)
            h = double_gelu(narrow(z))
            for r in range(SUB):
                at = r * groups * LANES
                one[k, :, at : at + groups * LANES] = h[units * r : units * (r + 1)]
        pairs(t + 1)
        return carry

    pairs(0)
    lax.fori_loop(0, blocks * turns + 2, step, 0)

    def close(b, carry):
        done = {}
        for r in range(SUB):
            for g in range(groups):
                at = (r * groups + g) * LANES
                row = SUB * g + r
                count = counts_ref[pl.ds(b * block + row, 1), :].astype(jnp.float32)
                done[row] = total[b, :, at : at + LANES] * (SCALE / count)
                if not grouped:
                    out_ref[b * block + row] = done[row]
        if grouped:
            for q in range(channels // SUB):
                out_ref[q, pl.ds(pl.multiple_of(b * block * SUB, SUB * SUB), block * SUB), :] = narrow(
                    jnp.concatenate(
                        [done[row][SUB * q : SUB * (q + 1)] for row in range(block)], axis=0
                    )
                )
        return carry

    lax.fori_loop(0, blocks, close, 0)


def encode(counts, table, codes, first, middle, final, cells, grouped):
    rows = counts.shape[0]
    units = middle.shape[0]
    channels = final.shape[0]
    block = min(2 * SUB, rows)
    per = final.shape[1] // units
    if grouped:
        shape = jax.ShapeDtypeStruct((channels // SUB, rows * SUB, LANES), jnp.bfloat16)
    else:
        shape = jax.ShapeDtypeStruct((rows, channels, LANES), jnp.float32)
    vmem = lambda: pl.BlockSpec(memory_space=pltpu.VMEM)
    return pl.pallas_call(
        functools.partial(encoder_kernel, cells, grouped),
        out_shape=shape,
        in_specs=[vmem() for _ in range(6)],
        out_specs=vmem(),
        scratch_shapes=[
            pltpu.VMEM((per, first.shape[1], block // SUB * LANES), jnp.bfloat16),
            pltpu.VMEM((per, units, block * LANES), jnp.bfloat16),
            pltpu.VMEM((per * units, block * LANES), jnp.bfloat16),
            pltpu.VMEM((rows // block, channels, block * LANES), jnp.float32),
        ],
        compiler_params=pltpu.CompilerParams(vmem_limit_bytes=56 * 1024 * 1024),
    )(counts, table, codes, first, middle, final)


def prepare_kernel(
    sizes, *refs
):
    inputs, refs = refs[:5], refs[5:]
    out_ref, codes, first, middle, final = refs[:5]
    near, send, recv, fetched = refs[5:9]
    local = refs[9:]
    fetches = [
        pltpu.make_async_copy(source, target, fetched.at[n])
        for n, (source, target) in enumerate(zip(inputs, local))
    ]
    for fetch in fetches:
        fetch.start()
    points_ref, neighbours_ref, in_ref, mid_ref, last_ref = local
    places = [lax.axis_index(a) for a in ("gx", "gy", "gz")]
    widths = [min(n, 3) for n in sizes]
    home = [1 if n > 2 else 0 for n in sizes]
    blocks = [
        (x, y, z) for x in range(widths[0]) for y in range(widths[1]) for z in range(widths[2])
    ]
    number = lambda b: (b[0] * widths[1] + b[1]) * widths[2] + b[2]

    def reader(block):
        there = [lax.rem(p - o + h + n, n) for p, o, h, n in zip(places, block, home, sizes)]
        return dict(zip(("gx", "gy", "gz"), there))

    others = [b for b in blocks if list(b) != home]
    barrier = pltpu.get_barrier_semaphore()
    for block in others:
        pl.semaphore_signal(
            barrier, inc=1, device_id=reader(block), device_id_type=pl.DeviceIdType.MESH
        )
    pl.semaphore_wait(barrier, len(others))
    fetches[0].wait()
    copies = {}
    for block in others:
        b = number(block)
        copies[b] = pltpu.make_async_remote_copy(
            src_ref=points_ref,
            dst_ref=near.at[b],
            send_sem=send.at[b],
            recv_sem=recv.at[b],
            device_id=reader(block),
            device_id_type=pl.DeviceIdType.MESH,
        )
        copies[b].start()
    place_x, place_y, place_z = places
    count_x, count_y, count_z = sizes
    per_device = points_ref.shape[0] * LANES // in_ref.shape[0]
    cells_x, cells_y, cells_z, slots = neighbours_ref.shape
    rows_y = LANES // cells_z
    rows = codes.shape[0] // slots
    for fetch in fetches[1:]:
        fetch.wait()
    units = mid_ref.shape[0]
    words = in_ref.shape[0] // 3
    per = final.shape[1] // units
    iota = lambda shape, d: lax.broadcasted_iota(jnp.int32, shape, d)
    spread = jnp.where(iota((SUB * units, units), 0) % units == iota((SUB * units, units), 1), 1.0, 0.0)
    values = 3 * words
    wide = jnp.where(iota((values, values * SUB), 0) == iota((values, values * SUB), 1) // SUB, 1.0, 0.0)
    narrow = lambda a: a.astype(jnp.bfloat16)
    inputs = in_ref[...].astype(jnp.float32).T
    tiled = jnp.dot(narrow(inputs), narrow(wide), preferred_element_type=jnp.float32)
    tiled = jnp.dot(narrow(spread), narrow(tiled), preferred_element_type=jnp.float32)
    shape = (SUB * units, values * SUB)
    first[...] = narrow(jnp.where(iota(shape, 0) // units == iota(shape, 1) % SUB, tiled, 0.0))
    middle[...] = narrow(mid_ref[...].astype(jnp.float32).T * 0.5)
    turned = narrow(last_ref[...].astype(jnp.float32) * 0.5)
    for k in range(per):
        final[:, units * k : units * (k + 1)] = turned
    width_y, width_z = widths[1:]
    def prepare(row, carry):
        strip, x = row // cells_x, lax.rem(row, cells_x)
        near = neighbours_ref[x, pl.ds(strip * rows_y, rows_y)].reshape(LANES, slots).T
        owner = over(near, per_device)
        at_z = offset(within(owner, count_z), place_z, count_z)
        at_y = offset(within(over(owner, count_z), count_y), place_y, count_y)
        at_x = offset(over(owner, count_z * count_y), place_x, count_x)
        code = ((at_x * width_y + at_y) * width_z + at_z) * per_device + within(near, per_device)
        codes[pl.ds(pl.multiple_of(row * slots, SUB), slots), :] = code
        return carry

    lax.fori_loop(0, rows, prepare, 0, unroll=min(8, rows))
    pieces = per_device // LANES
    for block in [tuple(home)] + others:
        b = number(block)
        if b in copies:
            copies[b].wait()
            values = near[b]
        else:
            values = points_ref[...]
        fine = jnp.round(values * FINE).astype(jnp.int32)
        coarse = jnp.round(values * COARSE).astype(jnp.int32)
        for w in range(words):
            at = lambda v: slice(pieces * (3 * w + v), pieces * (3 * w + v + 1))
            out_ref[w, pieces * b : pieces * (b + 1), :] = (
                fine[at(0)] * 2097152 + (fine[at(1)] + 1024) * 1024 + (coarse[at(2)] + 512)
            )


def prepare(points, neighbours, kernel_in, kernel_mid, kernel_out):
    sizes = tuple(lax.axis_size(a) for a in ("gx", "gy", "gz"))
    blocks = math.prod(min(n, 3) for n in sizes)
    units, channels = kernel_out.shape
    values = kernel_in.shape[0]
    per = 2
    vmem = lambda: pl.BlockSpec(memory_space=pltpu.VMEM)
    shapes = [
        ((values // 3, blocks * points.size // values // LANES, LANES), jnp.int32),
        ((neighbours.size // LANES, LANES), jnp.int32),
        ((SUB * units, values * SUB), jnp.bfloat16),
        ((units, units), jnp.bfloat16),
        ((channels, per * units), jnp.bfloat16),
    ]
    arrays = (points.reshape(-1, LANES), neighbours, kernel_in, kernel_mid, kernel_out.T)
    return pl.pallas_call(
        functools.partial(prepare_kernel, sizes),
        out_shape=[jax.ShapeDtypeStruct(*shape) for shape in shapes],
        in_specs=[pl.BlockSpec(memory_space=pltpu.HBM) for _ in arrays],
        out_specs=[vmem() for _ in shapes],
        scratch_shapes=[
            pltpu.VMEM((blocks, points.size // LANES, LANES), jnp.float32),
            pltpu.SemaphoreType.DMA((blocks,)),
            pltpu.SemaphoreType.DMA((blocks,)),
            pltpu.SemaphoreType.DMA((len(arrays),)),
        ]
        + [pltpu.VMEM(a.shape, a.dtype) for a in arrays],
        compiler_params=pltpu.CompilerParams(
            collective_id=1, has_side_effects=True, vmem_limit_bytes=62 * 1024 * 1024
        ),
    )(*arrays)


def lane_maps(quarters, parts, inner_k, inner_j):
    grid = np.indices((quarters, 2, parts, inner_k, inner_j)).reshape(5, -1)
    return grid[0] * inner_j + grid[4], grid[2] * inner_k + grid[3], grid[1]


def spectral_tables(count_x, count_y, count_z, cells_x, cells_y, cells_z, group):
    keep = MODES
    signed = np.where(np.arange(keep) < keep // 2, np.arange(keep), np.arange(keep) - keep)
    mode_j, mode_k, imaginary = lane_maps(count_x, count_y, keep // count_y, keep // count_x)
    turn = 2.0 * np.pi / GRID
    rows_y = LANES // cells_z
    place_z, row_y, cell_z = np.indices((count_z, rows_y, cells_z)).reshape(3, -1)
    phase = turn * (
        (signed[mode_j] * row_y[:, None] + mode_k * (place_z * cells_z + cell_z)[:, None]) % GRID
    )
    forward = np.where(imaginary, -np.sin(phase), np.cos(phase))
    weight = np.where(mode_k == 0, 1.0, 2.0)
    inverse = (np.where(imaginary, -np.sin(phase), np.cos(phase)) * weight).T
    sign = np.where(imaginary, -1.0, 1.0)
    strip = turn * ((signed[mode_j] * (rows_y * np.arange(GRID // rows_y))[:, None]) % GRID)
    strips = np.stack([np.cos(strip), np.sin(strip) * sign])
    cell = np.arange(count_x * cells_x).reshape(count_x, 1, cells_x)
    angle = turn * ((signed[:, None] * cell) % GRID)
    eye = np.eye(group)

    def expand(values):
        wide = np.einsum("pab,cd->pacbd", values, eye)
        return wide.reshape(count_x, values.shape[1] * group, values.shape[2] * group)

    ahead = np.concatenate([expand(np.cos(angle)), expand(np.sin(angle))], axis=2)
    back = np.swapaxes(angle, 1, 2)
    back = np.concatenate([expand(np.cos(back)), expand(np.sin(back))], axis=2)
    partner = (keep - mode_j) % keep
    same = (
        (mode_j[:, None] == partner[None, :])
        & (mode_k[:, None] == 0)
        & (mode_k[None, :] == 0)
        & (imaginary[:, None] == imaginary[None, :])
        & (mode_j[:, None] != keep // 2)
    )
    flip = same * sign[None, :]
    power = np.where(mode_k == 0, 0.5, 2.0)
    lanes = np.stack([sign, power])
    narrow = lambda array: jnp.asarray(array.astype(np.float32), jnp.bfloat16)
    single = lambda array: jnp.asarray(array.astype(np.float32))
    return (
        narrow(forward),
        narrow(inverse),
        single(strips),
        narrow(ahead),
        narrow(back),
        narrow(flip),
        single(lanes),
    )


def swap_halves(values):
    return jnp.concatenate(
        [
            pltpu.roll(values[:, at : at + LANES], LANES // 2, 1)
            for at in range(0, values.shape[1], LANES)
        ],
        axis=1,
    )


def split(values):
    upper = values.astype(jnp.bfloat16)
    return upper, (values - upper.astype(jnp.float32)).astype(jnp.bfloat16)


def spectral_kernel(
    count_x,
    count_y,
    count_z,
    lat_ref,
    weight_ref,
    forward_ref,
    inverse_ref,
    strips_ref,
    ahead_ref,
    back_ref,
    flip_ref,
    lanes_ref,
    out_ref,
    came,
    plane,
    sums,
    sums_in,
    own,
    own_in,
    turned,
    mixed,
    mixed_in,
    joined,
    all_modes,
    pieces,
    send_a, recv_a, send_b, recv_b, send_c, recv_c, send_d, recv_d, send_e, recv_e, send_f, recv_f,
):
    place_x, place_y, place_z = lax.axis_index("gx"), lax.axis_index("gy"), lax.axis_index("gz")
    members = count_y * count_z
    me = place_y * count_z + place_z
    group = SUB
    strip_rows = plane.shape[0]
    half_modes = MODES // count_z
    inner = (MODES // count_x) * (MODES // count_y)
    mesh_id = pl.DeviceIdType.MESH

    def member(t):
        other = lax.rem(me + t, members)
        return other, {"gy": other // count_z, "gz": lax.rem(other, count_z)}

    def column(t):
        other = lax.rem(place_x + t, count_x)
        return other, {"gx": other}

    barrier = pltpu.get_barrier_semaphore()
    for t in range(1, members):
        pl.semaphore_signal(barrier, inc=1, device_id=member(t)[1], device_id_type=mesh_id)
    for t in range(1, count_x):
        pl.semaphore_signal(barrier, inc=1, device_id=column(t)[1], device_id_type=mesh_id)
    pl.semaphore_wait(barrier, members - 1 + count_x - 1)

    def exchange_with(peer, total, source, target, send, recv):
        copies = []
        for t in range(1, total):
            other, device = peer(t)
            copy = pltpu.make_async_remote_copy(
                src_ref=source(other),
                dst_ref=target,
                send_sem=send.at[t],
                recv_sem=recv.at[t],
                device_id=device,
                device_id_type=mesh_id,
            )
            copy.start()
            copies.append(copy)
        return copies

    def apart(d, e):
        other = {
            "gy": lax.rem(place_y + count_y - d, count_y),
            "gz": lax.rem(place_z + e, count_z),
        }
        return other["gy"] * count_z + other["gz"], other

    def send_to(d, e, source, target, send, recv):
        other, device = apart(d, e)
        copy = pltpu.make_async_remote_copy(
            src_ref=source.at[other],
            dst_ref=target.at[me],
            send_sem=send.at[d * count_z + e],
            recv_sem=recv.at[d * count_z + e],
            device_id=device,
            device_id_type=mesh_id,
        )
        copy.start()
        return copy

    steps = [(d, e) for d in range(count_y) for e in range(count_z)]
    arrivals = {s: send_to(*s, lat_ref, came, send_a, recv_a) for s in steps if s != (0, 0)}
    came[me] = lat_ref[me]
    sign = lanes_ref[0:1, :]
    plane[...] = jnp.zeros_like(plane)
    chunks = came.shape[1] // strip_rows

    def ahead_step(source, chunk, carry):
        strip = source * chunks + chunk
        at = pl.multiple_of(chunk * strip_rows, strip_rows)
        block = jnp.concatenate(
            [came[source * count_z + z, pl.ds(at, strip_rows), :] for z in range(count_z)], axis=1
        )
        part = jnp.dot(block, forward_ref[...], preferred_element_type=jnp.float32)
        cosine = strips_ref[0, pl.ds(strip, 1), :]
        sine = strips_ref[1, pl.ds(strip, 1), :]
        plane[...] += part * cosine + swap_halves(part) * sine
        return carry

    for d in range(count_y):
        for e in range(count_z):
            if (d, e) in arrivals:
                arrivals[d, e].wait()
        source = lax.rem(place_y + d, count_y)
        lax.fori_loop(0, chunks, functools.partial(ahead_step, source), 0)
    lane_ids = lax.broadcasted_iota(jnp.int32, (strip_rows, LANES), 1)
    for q in range(count_x):
        part = plane[:, LANES * q : LANES * (q + 1)]
        if q == 0:
            rest = part - part.astype(jnp.bfloat16).astype(jnp.float32)
            part = jnp.where(lane_ids == LANES // 2, pltpu.roll(rest, LANES // 2, 1), part)
        sums[q] = part.astype(jnp.bfloat16)
    copies = exchange_with(column, count_x, lambda p: sums.at[p], sums_in.at[place_x], send_b, recv_b)
    sums_in[place_x] = sums[place_x]
    for copy in copies:
        copy.wait()
    constant_lane = jnp.logical_and(lane_ids == 0, place_x == 0)
    rest_lane = jnp.logical_and(lane_ids == LANES // 2, place_x == 0)
    spectrum = None
    for q in range(count_x):
        part = sums_in[q].astype(jnp.float32)
        part = part + jnp.where(constant_lane, pltpu.roll(part, LANES // 2, 1), 0.0)
        part = jnp.where(rest_lane, 0.0, part)
        for piece in split(part):
            turn = pltpu.roll(piece.astype(jnp.float32), LANES // 2, 1) * sign[:, :LANES]
            term = jnp.dot(
                ahead_ref[q],
                jnp.concatenate([piece, turn.astype(jnp.bfloat16)], axis=0),
                preferred_element_type=jnp.float32,
            )
            spectrum = term if spectrum is None else spectrum + term
    half_rows = half_modes * group
    for z in range(count_z):
        own[z] = spectrum[half_rows * z : half_rows * (z + 1)].astype(jnp.bfloat16)

    copies = exchange_with(
        member, members, lambda p: own.at[lax.rem(p, count_z)], own_in.at[me], send_c, recv_c
    )
    own_in[me] = own[place_z]
    mixed_rows = lax.broadcasted_iota(jnp.int32, (2 * inner, LANES), 0) % inner
    mixed_lanes = lax.broadcasted_iota(jnp.int32, (2 * inner, LANES), 1) // (LANES // 2)
    modes_j = MODES // count_x
    modes_k = MODES // count_y
    row_mode = (mixed_rows % modes_j) * modes_k + mixed_rows // modes_j
    first_place = (place_x + place_y + place_z) == 0
    mode_zero = lax.broadcasted_iota(jnp.int32, (inner, LANES // 2), 0) == 0
    turned[...] = jnp.zeros_like(turned)
    for copy in copies:
        copy.wait()
    arrived = [own_in[p].astype(jnp.float32) for p in range(members)]
    for i in range(half_modes):
        column_values = jnp.concatenate([a[group * i : group * (i + 1)] for a in arrived], axis=0)
        column_values = jnp.concatenate([column_values, column_values], axis=0)
        mixed[i] = column_values.T
        at = pl.multiple_of(place_y * inner, inner)
        both = jnp.concatenate(
            [mixed[i, pl.ds(at, inner), :], mixed[i, pl.ds(LANES // 2 + at, inner), :]], axis=0
        )
        wide = jnp.concatenate(
            [
                jnp.where(row_mode == 2 * t + mixed_lanes, both, 0.0).astype(jnp.bfloat16)
                for t in range(inner // 2)
            ],
            axis=1,
        )
        by_real = jnp.dot(wide, weight_ref[0, i], preferred_element_type=jnp.float32)
        by_imag = jnp.dot(wide, weight_ref[1, i], preferred_element_type=jnp.float32)
        real = by_real[:inner] - by_imag[inner:]
        imag = by_imag[:inner] + by_real[inner:]
        if i == 0:
            drop = jnp.logical_and(mode_zero, first_place)
            real = jnp.where(drop, 0.0, real)
            imag = jnp.where(drop, 0.0, imag)
        turned[i, pl.ds(at, inner), 0 : LANES // 2] = real
        turned[i, pl.ds(LANES // 2 + at, inner), 0 : LANES // 2] = imag
    flat = [turned[i].T for i in range(half_modes)]
    for p in range(members):
        joined[p] = jnp.concatenate(
            [f[group * p : group * (p + 1)] for f in flat], axis=0
        ).astype(jnp.bfloat16)

    copies = exchange_with(member, members, lambda p: joined.at[p], mixed_in.at[me], send_d, recv_d)
    mixed_in[me] = joined[me]
    for copy in copies:
        copy.wait()
    parts = []
    for z in range(count_z):
        value = mixed_in[z].astype(jnp.float32)
        for y in range(1, count_y):
            value = value + mixed_in[y * count_z + z].astype(jnp.float32)
        parts.append(value)
    all_modes[place_x] = jnp.concatenate(parts, axis=0).astype(jnp.bfloat16)
    copies = exchange_with(
        column, count_x, lambda p: all_modes.at[place_x], all_modes.at[place_x], send_e, recv_e
    )
    for copy in copies:
        copy.wait()
    modes = jnp.concatenate([all_modes[q] for q in range(count_x)], axis=1)
    scaled = modes.astype(jnp.float32) * (1.0 / GRID**3)
    partner = jnp.dot(modes, flip_ref[...], preferred_element_type=jnp.float32) * (1.0 / GRID**3)
    energy = None
    for i in range(MODES):
        value = scaled[group * i : group * (i + 1)]
        term = value * value * lanes_ref[1:2, :]
        if i != MODES // 2:
            other = (MODES - i) % MODES
            term = term + 0.5 * value * partner[group * other : group * (other + 1)]
        energy = term if energy is None else energy + term
    variance = jnp.sum(energy, axis=1, keepdims=True)
    gain = 1.0 / jnp.sqrt(variance + NORM_FLOOR)
    rotated = (swap_halves(scaled * float(GRID**3)) * -sign).astype(jnp.bfloat16)
    back = jnp.dot(
        back_ref[place_x], jnp.concatenate([modes, rotated], axis=0), preferred_element_type=jnp.float32
    )
    back = back.reshape(-1, group, back.shape[1]) * (gain * (1.0 / GRID**3))[None]
    plane[...] = back.reshape(plane.shape)

    def back_step(source, chunk, carry):
        strip = source * chunks + chunk
        at = pl.multiple_of(chunk * strip_rows, strip_rows)
        cosine = strips_ref[0, pl.ds(strip, 1), :]
        sine = strips_ref[1, pl.ds(strip, 1), :]
        value = plane[...]
        value = (value * cosine - swap_halves(value) * sine).astype(jnp.bfloat16)
        result = jnp.dot(value, inverse_ref[...], preferred_element_type=jnp.float32)
        for z in range(count_z):
            pieces[source * count_z + z, pl.ds(at, strip_rows), :] = result[
                :, LANES * z : LANES * (z + 1)
            ].astype(jnp.bfloat16)
        return carry

    copies = []
    for d in [*range(1, count_y), 0]:
        source = lax.rem(place_y + count_y - d, count_y)
        lax.fori_loop(0, chunks, functools.partial(back_step, source), 0)
        copies += [
            send_to(d, e, pieces, out_ref, send_f, recv_f) for e in range(count_z) if (d, e) != (0, 0)
        ]
    out_ref[me] = pieces[me]
    for copy in copies:
        copy.wait()


def spectral_branch(lat, spectral):
    count_x, count_y, count_z = (lax.axis_size(a) for a in ("gx", "gy", "gz"))
    members, piece_rows, _ = lat.shape
    cells_x, cells_y, cells_z = GRID // count_x, GRID // count_y, GRID // count_z
    strip_rows = cells_x * SUB
    half_modes = MODES // count_z
    channels = spectral.shape[-1]
    inner = (MODES // count_x) * (MODES // count_y)
    lanes = 2 * MODES * MODES
    tables = spectral_tables(count_x, count_y, count_z, cells_x, cells_y, cells_z, SUB)
    weight = spectral.reshape(2, half_modes, inner * channels, channels)
    vmem = lambda: pl.BlockSpec(memory_space=pltpu.VMEM)
    half = half_modes * SUB
    dma = pltpu.SemaphoreType.DMA
    return pl.pallas_call(
        functools.partial(spectral_kernel, count_x, count_y, count_z),
        out_shape=jax.ShapeDtypeStruct(lat.shape, jnp.bfloat16),
        in_specs=[vmem() for _ in range(9)],
        out_specs=vmem(),
        scratch_shapes=[
            pltpu.VMEM(lat.shape, jnp.bfloat16),
            pltpu.VMEM((strip_rows, lanes), jnp.float32),
            pltpu.VMEM((count_x, strip_rows, LANES), jnp.bfloat16),
            pltpu.VMEM((count_x, strip_rows, LANES), jnp.bfloat16),
            pltpu.VMEM((count_z, half, LANES), jnp.bfloat16),
            pltpu.VMEM((members, half, LANES), jnp.bfloat16),
            pltpu.VMEM((half_modes, LANES, LANES), jnp.float32),
            pltpu.VMEM((half_modes, LANES, LANES), jnp.float32),
            pltpu.VMEM((members, half, LANES), jnp.bfloat16),
            pltpu.VMEM((members, half, LANES), jnp.bfloat16),
            pltpu.VMEM((count_x, MODES * SUB, LANES), jnp.bfloat16),
            pltpu.VMEM(lat.shape, jnp.bfloat16),
        ]
        + [dma((members,))] * 2
        + [dma((count_x,))] * 2
        + [dma((members,))] * 2
        + [dma((members,))] * 2
        + [dma((count_x,))] * 2
        + [dma((members,))] * 2,
        compiler_params=pltpu.CompilerParams(
            collective_id=0, has_side_effects=True, vmem_limit_bytes=48 * 1024 * 1024
        ),
    )(lat, weight, *tables)


def final_kernel(branch_ref, lat_ref, skip_ref, out_ref):
    members = branch_ref.shape[0]
    count = out_ref.shape[0]
    rows = count * SUB
    part = pl.ds(pl.multiple_of(pl.program_id(0) * rows, rows), rows)
    branch = [branch_ref[p, part, :].astype(jnp.float32) for p in range(members)]
    latent = [lat_ref[p, part, :].astype(jnp.float32) for p in range(members)]
    pick = lambda parts, x: jnp.concatenate([a[SUB * x : SUB * (x + 1)] for a in parts], axis=0)
    wide = jnp.concatenate([pick(latent, x) for x in range(count)], axis=1).astype(jnp.bfloat16)
    turned = skip_ref[...].astype(jnp.float32).T.astype(jnp.bfloat16)
    skip = jnp.dot(turned, wide, preferred_element_type=jnp.float32)
    for x in range(count):
        v = pick(branch, x) + skip[:, LANES * x : LANES * (x + 1)]
        inner = v * (0.7978845608028654 + 0.035677408136300125 * (v * v))
        half = 0.5 * v
        out_ref[x, 0] = (half + half * jnp.tanh(inner)).T


def finish(branch, lat, skip_weight, cells_x):
    members, piece_rows, _ = lat.shape
    channels = skip_weight.shape[0]
    rows = cells_x * SUB
    whole = pl.BlockSpec(memory_space=pltpu.VMEM)
    return pl.pallas_call(
        final_kernel,
        grid=(piece_rows // rows,),
        out_shape=jax.ShapeDtypeStruct((cells_x, piece_rows // rows, LANES, channels), jnp.float32),
        in_specs=[whole, whole, whole],
        out_specs=pl.BlockSpec((cells_x, 1, LANES, channels), lambda i: (0, i, 0, 0)),
        compiler_params=pltpu.CompilerParams(vmem_limit_bytes=24 * 1024 * 1024),
    )(branch, lat, skip_weight)


def summed_over_axes(values, axes):
    for axis in axes:
        count = lax.axis_size(axis)
        copies = jnp.broadcast_to(values[None], (count,) + values.shape)
        values = jnp.sum(lax.all_to_all(copies, axis, 0, 0, tiled=True), axis=0)
    return values


def exchange(values, axis, split_axis, concat_axis):
    return lax.all_to_all(
        values.astype(jnp.bfloat16), axis, split_axis=split_axis, concat_axis=concat_axis, tiled=True
    ).astype(jnp.float32)


def body(point_data, neighbours, counts, kernel_in, kernel_mid, kernel_out, spectral, skip_weight):
    count_y = lax.axis_size("gy")
    count_z = lax.axis_size("gz")
    place_x = lax.axis_index("gx")
    place_y = lax.axis_index("gy")
    place_z = lax.axis_index("gz")
    geometry_count, cells_x, cells_y, cells_z = neighbours.shape[0:4]
    per_device = point_data.shape[2]
    channels = skip_weight.shape[0]
    rows_y = LANES // cells_z
    shape = (cells_x, cells_y, cells_z)
    node_order = lambda values: jnp.swapaxes(
        values.reshape(cells_x, cells_y // rows_y, LANES), 0, 1
    ).reshape(-1, LANES)
    grouped = (
        count_y * count_z * SUB == channels
        and cells_x * SUB == LANES
        and count_z * MODES // 2 == MODES
        and 2 * (MODES // lax.axis_size("gx")) * MODES == LANES
    )
    latent = []
    for geometry in range(geometry_count):
        latent.append(
            encode(
                node_order(counts[geometry]),
                *prepare(
                    point_data[geometry], neighbours[geometry], kernel_in, kernel_mid, kernel_out
                ),
                shape,
                grouped,
            )
        )
    if grouped:
        results = [
            finish(spectral_branch(lat, spectral), lat, skip_weight, cells_x) for lat in latent
        ]
        return jnp.stack(results).reshape(geometry_count, cells_x, cells_y, cells_z, channels)
    latent = jnp.swapaxes(jnp.stack(latent), 2, 3).astype(jnp.bfloat16)
    latent = latent.reshape(geometry_count, cells_y // rows_y, cells_x, LANES, channels)
    latent = jnp.swapaxes(latent, 1, 2)
    latent = latent.reshape(geometry_count, cells_x, cells_y, cells_z, channels)
    cos_centred, sin_centred = tables(GRID, MODES, True)
    cos_third, sin_third = tables(GRID, MODES, False)
    back_cos, back_sin = third_weights(cos_third, sin_third, GRID)
    depth_full = lax.all_to_all(latent, "gz", split_axis=4, concat_axis=3, tiled=True)
    real_part, imag_part = forward_real(
        depth_full.astype(jnp.float32), cos_third, sin_third, "gxyzc,kz->gxykc"
    )
    real_part, imag_part = (
        lax.all_to_all(real_part, "gy", split_axis=3, concat_axis=2, tiled=True),
        lax.all_to_all(imag_part, "gy", split_axis=3, concat_axis=2, tiled=True),
    )
    real_part, imag_part = forward_complex(
        real_part, imag_part, cos_centred, sin_centred, "gxykc,jy->gxjkc"
    )
    real_part, imag_part = (
        lax.all_to_all(real_part, "gx", split_axis=2, concat_axis=1, tiled=True),
        lax.all_to_all(imag_part, "gx", split_axis=2, concat_axis=1, tiled=True),
    )
    real_part, imag_part = forward_complex(
        real_part, imag_part, cos_centred, sin_centred, "gxjkc,ix->gijkc"
    )
    spec_real, spec_imag = (
        exchange(real_part, "gz", split_axis=1, concat_axis=4),
        exchange(imag_part, "gz", split_axis=1, concat_axis=4),
    )
    spec_real = spec_real.astype(jnp.bfloat16)
    spec_imag = spec_imag.astype(jnp.bfloat16)
    mixed_real = jnp.einsum(
        "gijkc,ijkco->gijko", spec_real, spectral[0], preferred_element_type=jnp.float32
    ) - jnp.einsum("gijkc,ijkco->gijko", spec_imag, spectral[1], preferred_element_type=jnp.float32)
    mixed_imag = jnp.einsum(
        "gijkc,ijkco->gijko", spec_real, spectral[1], preferred_element_type=jnp.float32
    ) + jnp.einsum("gijkc,ijkco->gijko", spec_imag, spectral[0], preferred_element_type=jnp.float32)
    first_place = (place_x + place_y + place_z) == 0
    modes = mixed_real.shape[1:4]
    order = sum(lax.broadcasted_iota(jnp.int32, modes, d) for d in range(3))
    zero_mode = ((order == 0) & first_place)[None, ..., None]
    mixed_real = jnp.where(zero_mode, 0.0, mixed_real)
    mixed_imag = jnp.where(zero_mode, 0.0, mixed_imag)
    mixed_real = mixed_real.astype(jnp.bfloat16)
    mixed_imag = mixed_imag.astype(jnp.bfloat16)
    real_part, imag_part = (
        exchange(mixed_real, "gz", split_axis=4, concat_axis=1),
        exchange(mixed_imag, "gz", split_axis=4, concat_axis=1),
    )
    real_part, imag_part = inverse_complex(
        real_part.astype(jnp.float32),
        imag_part.astype(jnp.float32),
        cos_centred,
        sin_centred,
        "gijkc,ix->gxjkc",
    )
    real_part, imag_part = (
        exchange(real_part, "gx", split_axis=1, concat_axis=2),
        exchange(imag_part, "gx", split_axis=1, concat_axis=2),
    )
    real_part, imag_part = inverse_complex(
        real_part, imag_part, cos_centred, sin_centred, "gxjkc,jy->gxykc"
    )
    real_part, imag_part = (
        exchange(real_part, "gy", split_axis=2, concat_axis=3),
        exchange(imag_part, "gy", split_axis=2, concat_axis=3),
    )
    depth_part = inverse_real(real_part, imag_part, back_cos, back_sin, "gxykc,kz->gxyzc")
    branch = exchange(depth_part, "gz", split_axis=3, concat_axis=4)
    skip = jnp.einsum("gxyzc,co->gxyzo", latent, skip_weight, preferred_element_type=jnp.float32)
    cells_total = float(GRID**3)
    variance = (
        summed_over_axes(jnp.sum(branch * branch, axis=(1, 2, 3)), ("gz", "gy", "gx")) / cells_total
    )
    normed = branch / jnp.sqrt(variance + NORM_FLOOR)[:, None, None, None, :]
    return jax.nn.gelu(normed + skip, approximate=True)


def solution(mesh):
    in_specs = (
        P(None, None, ("gx", "gy", "gz")),
        P(None, "gx", "gy", "gz", None),
        P(None, "gx", "gy", "gz"),
        P(),
        P(),
        P(),
        P(None, "gz", "gx", "gy", None, None),
        P(),
    )
    out_specs = P(None, "gx", "gy", "gz", None)
    return jax.shard_map(body, mesh=mesh, in_specs=in_specs, out_specs=out_specs, check_vma=False)
```

```python
import functools
import math

import jax
import jax.numpy as jnp
import numpy as np
from jax import lax
from jax.experimental import pallas as pl
from jax.experimental.pallas import tpu as pltpu
from jax.sharding import PartitionSpec as P

GRID = 64
MODES = 16
NB = 32


HIGH = lax.Precision.HIGH
NORM_FLOOR = 1.0


def tables(length, keep_count, centred):
    position = jnp.arange(length, dtype=jnp.int32)
    frequency = jnp.arange(keep_count, dtype=jnp.int32)
    if centred:
        frequency = jnp.where(
            frequency < keep_count // 2, frequency, frequency + length - keep_count
        )
    phases = frequency[:, None] * position[None, :] % length
    angles = phases.astype(jnp.float32) * (2.0 * math.pi / length)
    return (jnp.cos(angles), jnp.sin(angles))


def third_weights(cos_table, sin_table, length):
    factor = (
        jnp.where(jnp.arange(cos_table.shape[0]) == 0, 1.0, 2.0).astype(jnp.float32)[:, None]
        / length**3
    )
    return (cos_table * factor, sin_table * factor)


def contract(pattern, operand, table):
    return jnp.einsum(pattern, operand, table, precision=HIGH)


def forward_real(values, cos_table, sin_table, pattern):
    return (contract(pattern, values, cos_table), -contract(pattern, values, sin_table))


def forward_complex(real_part, imag_part, cos_table, sin_table, pattern):
    new_real = contract(pattern, real_part, cos_table) + contract(pattern, imag_part, sin_table)
    new_imag = contract(pattern, imag_part, cos_table) - contract(pattern, real_part, sin_table)
    return (new_real, new_imag)


def inverse_complex(real_part, imag_part, cos_table, sin_table, pattern):
    new_real = contract(pattern, real_part, cos_table) - contract(pattern, imag_part, sin_table)
    new_imag = contract(pattern, real_part, sin_table) + contract(pattern, imag_part, cos_table)
    return (new_real, new_imag)


def inverse_real(real_part, imag_part, cos_table, sin_table, pattern):
    return contract(pattern, real_part, cos_table) - contract(pattern, imag_part, sin_table)


SUB = 8
LANES = 128
SCALE = 0.035677408136300125 ** (-1.0 / 3.0)
SHIFT = 0.7978845608028654 * SCALE
FINE = 1023.0
COARSE = 511.0


def double_gelu(y):
    return y + y * jnp.tanh(y * (y * y + jnp.asarray(SHIFT, y.dtype)))


def pick(leaf, bits, low, high, level):
    if high - low == 1:
        return leaf(low)
    half = 1 << (level - 1)
    if low + half >= high:
        return pick(leaf, bits, low, high, level - 1)
    first = pick(leaf, bits, low, low + half, level - 1)
    second = pick(leaf, bits, low + half, high, level - 1)
    return jnp.where(bits[level - 1], second, first)


def over(values, count):
    return values >> (count.bit_length() - 1) if count & (count - 1) == 0 else values // count


def within(values, count):
    return values & (count - 1) if count & (count - 1) == 0 else lax.rem(values, count)


def offset(owner, place, count):
    return within(owner - place + (count + (1 if count > 2 else 0)), count)


def encoder_kernel(
    cells, grouped, counts_ref, table_ref, codes, first, middle, final, out_ref,
    stack, one, two, total,
):
    place_x, place_y, place_z = lax.axis_index("gx"), lax.axis_index("gy"), lax.axis_index("gz")
    cells_x, cells_y, cells_z = cells
    rows_y = LANES // cells_z
    rows = counts_ref.shape[0]
    slots = codes.shape[0] // rows
    units = middle.shape[0]
    channels = final.shape[0]
    words, table_rows = first.shape[1] // (3 * SUB), table_ref.shape[1]
    depth = max(1, (table_rows - 1).bit_length())
    per = stack.shape[0]
    block = total.shape[2] // LANES
    groups = block // SUB
    turns = slots // per
    blocks = rows // block
    iota = lambda shape, d: lax.broadcasted_iota(jnp.int32, shape, d)
    narrow = lambda a: a.astype(jnp.bfloat16)
    one[...] = jnp.zeros_like(one)
    two[...] = jnp.zeros_like(two)
    total[...] = jnp.zeros_like(total)
    lane_ids = iota((SUB, LANES), 1)
    sub_ids = iota((SUB, LANES), 0)
    centre = lambda cell: (cell.astype(jnp.float32) + 0.5) * (1.0 / (GRID * SCALE))
    centre_z = centre(place_z * cells_z + within(lane_ids, cells_z))
    centre_x = [
        centre(place_x * cells_x + within(SUB * g + sub_ids, cells_x)) for g in range(groups)
    ]
    lane_y = over(lane_ids, cells_z) + place_y * cells_y

    def pairs(t):
        here = jnp.minimum(t // turns, blocks - 1)
        turn = lax.rem(t, turns)
        limit = jnp.where(t < blocks * turns, 0, slots)
        centre_y = centre(lane_y + (here * block // cells_x) * rows_y)
        for k in range(per):
            slot = turn * per + k
            for g in range(groups):
                base = here * block + SUB * g
                code = codes[pl.ds(base * slots + slot, SUB, stride=slots), :]
                lane = code & (LANES - 1)
                bits = [(code & (LANES << b)) != 0 for b in range(depth)]
                live = slot + limit < counts_ref[pl.ds(pl.multiple_of(base, SUB), SUB), :]
                found = []
                for w in range(words):
                    leaf = lambda r: jnp.take_along_axis(
                        jnp.broadcast_to(table_ref[w, r : r + 1, :], (SUB, LANES)),
                        lane,
                        axis=1,
                        mode="promise_in_bounds",
                    )
                    word = pick(leaf, bits, 0, table_rows, depth)
                    found += [word >> 21, ((word >> 10) & 2047) - 1024, (word & 1023) - 512]
                parts = []
                for v, x in enumerate(found):
                    x = x.astype(jnp.float32) * (1.0 / (SCALE * (COARSE if v % 3 == 2 else FINE)))
                    if v < 3:
                        x = x - (centre_x[g], centre_y, centre_z)[v]
                    parts.append(jnp.where(live, x, 0.0))
                stack[k, :, LANES * g : LANES * (g + 1)] = narrow(jnp.concatenate(parts, axis=0))

    def step(t, carry):
        there = jnp.maximum(t - 2, 0) // turns
        total[there] += jnp.dot(final[...], two[...], preferred_element_type=jnp.float32)
        for k in range(per):
            z = jnp.dot(middle[...], one[k], preferred_element_type=jnp.float32)
            two[units * k : units * (k + 1), :] = double_gelu(narrow(z))
        for k in range(per):
            z = jnp.dot(first[...], stack[k], preferred_element_type=jnp.float32)
            h = double_gelu(narrow(z))
            for r in range(SUB):
                at = r * groups * LANES
                one[k, :, at : at + groups * LANES] = h[units * r : units * (r + 1)]
        pairs(t + 1)
        return carry

    pairs(0)
    lax.fori_loop(0, blocks * turns + 2, step, 0)

    def close(b, carry):
        done = {}
        for r in range(SUB):
            for g in range(groups):
                at = (r * groups + g) * LANES
                row = SUB * g + r
                count = counts_ref[pl.ds(b * block + row, 1), :].astype(jnp.float32)
                done[row] = total[b, :, at : at + LANES] * (SCALE / count)
                if not grouped:
                    out_ref[b * block + row] = done[row]
        if grouped:
            for q in range(channels // SUB):
                out_ref[q, pl.ds(pl.multiple_of(b * block * SUB, SUB * SUB), block * SUB), :] = narrow(
                    jnp.concatenate(
                        [done[row][SUB * q : SUB * (q + 1)] for row in range(block)], axis=0
                    )
                )
        return carry

    lax.fori_loop(0, blocks, close, 0)


def encode(counts, table, codes, first, middle, final, cells, grouped):
    rows = counts.shape[0]
    units = middle.shape[0]
    channels = final.shape[0]
    block = min(2 * SUB, rows)
    per = final.shape[1] // units
    if grouped:
        shape = jax.ShapeDtypeStruct((channels // SUB, rows * SUB, LANES), jnp.bfloat16)
    else:
        shape = jax.ShapeDtypeStruct((rows, channels, LANES), jnp.float32)
    vmem = lambda: pl.BlockSpec(memory_space=pltpu.VMEM)
    return pl.pallas_call(
        functools.partial(encoder_kernel, cells, grouped),
        out_shape=shape,
        in_specs=[vmem() for _ in range(6)],
        out_specs=vmem(),
        scratch_shapes=[
            pltpu.VMEM((per, first.shape[1], block // SUB * LANES), jnp.bfloat16),
            pltpu.VMEM((per, units, block * LANES), jnp.bfloat16),
            pltpu.VMEM((per * units, block * LANES), jnp.bfloat16),
            pltpu.VMEM((rows // block, channels, block * LANES), jnp.float32),
        ],
        compiler_params=pltpu.CompilerParams(vmem_limit_bytes=56 * 1024 * 1024),
    )(counts, table, codes, first, middle, final)


def prepare_kernel(
    sizes, *refs
):
    inputs, refs = refs[:5], refs[5:]
    out_ref, codes, first, middle, final = refs[:5]
    near, send, recv, fetched = refs[5:9]
    local = refs[9:]
    fetches = [
        pltpu.make_async_copy(source, target, fetched.at[n])
        for n, (source, target) in enumerate(zip(inputs, local))
    ]
    for fetch in fetches:
        fetch.start()
    points_ref, neighbours_ref, in_ref, mid_ref, last_ref = local
    places = [lax.axis_index(a) for a in ("gx", "gy", "gz")]
    widths = [min(n, 3) for n in sizes]
    home = [1 if n > 2 else 0 for n in sizes]
    blocks = [
        (x, y, z) for x in range(widths[0]) for y in range(widths[1]) for z in range(widths[2])
    ]
    number = lambda b: (b[0] * widths[1] + b[1]) * widths[2] + b[2]

    def reader(block):
        there = [lax.rem(p - o + h + n, n) for p, o, h, n in zip(places, block, home, sizes)]
        return dict(zip(("gx", "gy", "gz"), there))

    others = [b for b in blocks if list(b) != home]
    barrier = pltpu.get_barrier_semaphore()
    for block in others:
        pl.semaphore_signal(
            barrier, inc=1, device_id=reader(block), device_id_type=pl.DeviceIdType.MESH
        )
    pl.semaphore_wait(barrier, len(others))
    fetches[0].wait()
    copies = {}
    for block in others:
        b = number(block)
        copies[b] = pltpu.make_async_remote_copy(
            src_ref=points_ref,
            dst_ref=near.at[b],
            send_sem=send.at[b],
            recv_sem=recv.at[b],
            device_id=reader(block),
            device_id_type=pl.DeviceIdType.MESH,
        )
        copies[b].start()
    place_x, place_y, place_z = places
    count_x, count_y, count_z = sizes
    per_device = points_ref.shape[0] * LANES // in_ref.shape[0]
    cells_x, cells_y, cells_z, slots = neighbours_ref.shape
    rows_y = LANES // cells_z
    rows = codes.shape[0] // slots
    for fetch in fetches[1:]:
        fetch.wait()
    units = mid_ref.shape[0]
    words = in_ref.shape[0] // 3
    per = final.shape[1] // units
    iota = lambda shape, d: lax.broadcasted_iota(jnp.int32, shape, d)
    spread = jnp.where(iota((SUB * units, units), 0) % units == iota((SUB * units, units), 1), 1.0, 0.0)
    values = 3 * words
    wide = jnp.where(iota((values, values * SUB), 0) == iota((values, values * SUB), 1) // SUB, 1.0, 0.0)
    narrow = lambda a: a.astype(jnp.bfloat16)
    inputs = in_ref[...].astype(jnp.float32).T
    tiled = jnp.dot(narrow(inputs), narrow(wide), preferred_element_type=jnp.float32)
    tiled = jnp.dot(narrow(spread), narrow(tiled), preferred_element_type=jnp.float32)
    shape = (SUB * units, values * SUB)
    first[...] = narrow(jnp.where(iota(shape, 0) // units == iota(shape, 1) % SUB, tiled, 0.0))
    middle[...] = narrow(mid_ref[...].astype(jnp.float32).T * 0.5)
    turned = narrow(last_ref[...].astype(jnp.float32) * 0.5)
    for k in range(per):
        final[:, units * k : units * (k + 1)] = turned
    width_y, width_z = widths[1:]
    def prepare(row, carry):
        strip, x = row // cells_x, lax.rem(row, cells_x)
        near = neighbours_ref[x, pl.ds(strip * rows_y, rows_y)].reshape(LANES, slots).T
        owner = over(near, per_device)
        at_z = offset(within(owner, count_z), place_z, count_z)
        at_y = offset(within(over(owner, count_z), count_y), place_y, count_y)
        at_x = offset(over(owner, count_z * count_y), place_x, count_x)
        code = ((at_x * width_y + at_y) * width_z + at_z) * per_device + within(near, per_device)
        codes[pl.ds(pl.multiple_of(row * slots, SUB), slots), :] = code
        return carry

    lax.fori_loop(0, rows, prepare, 0, unroll=min(8, rows))
    pieces = per_device // LANES
    for block in [tuple(home)] + others:
        b = number(block)
        if b in copies:
            copies[b].wait()
            values = near[b]
        else:
            values = points_ref[...]
        fine = jnp.round(values * FINE).astype(jnp.int32)
        coarse = jnp.round(values * COARSE).astype(jnp.int32)
        for w in range(words):
            at = lambda v: slice(pieces * (3 * w + v), pieces * (3 * w + v + 1))
            out_ref[w, pieces * b : pieces * (b + 1), :] = (
                fine[at(0)] * 2097152 + (fine[at(1)] + 1024) * 1024 + (coarse[at(2)] + 512)
            )


def prepare(points, neighbours, kernel_in, kernel_mid, kernel_out):
    sizes = tuple(lax.axis_size(a) for a in ("gx", "gy", "gz"))
    blocks = math.prod(min(n, 3) for n in sizes)
    units, channels = kernel_out.shape
    values = kernel_in.shape[0]
    per = 2
    vmem = lambda: pl.BlockSpec(memory_space=pltpu.VMEM)
    shapes = [
        ((values // 3, blocks * points.size // values // LANES, LANES), jnp.int32),
        ((neighbours.size // LANES, LANES), jnp.int32),
        ((SUB * units, values * SUB), jnp.bfloat16),
        ((units, units), jnp.bfloat16),
        ((channels, per * units), jnp.bfloat16),
    ]
    arrays = (points.reshape(-1, LANES), neighbours, kernel_in, kernel_mid, kernel_out.T)
    return pl.pallas_call(
        functools.partial(prepare_kernel, sizes),
        out_shape=[jax.ShapeDtypeStruct(*shape) for shape in shapes],
        in_specs=[pl.BlockSpec(memory_space=pltpu.HBM) for _ in arrays],
        out_specs=[vmem() for _ in shapes],
        scratch_shapes=[
            pltpu.VMEM((blocks, points.size // LANES, LANES), jnp.float32),
            pltpu.SemaphoreType.DMA((blocks,)),
            pltpu.SemaphoreType.DMA((blocks,)),
            pltpu.SemaphoreType.DMA((len(arrays),)),
        ]
        + [pltpu.VMEM(a.shape, a.dtype) for a in arrays],
        compiler_params=pltpu.CompilerParams(
            collective_id=1, has_side_effects=True, vmem_limit_bytes=62 * 1024 * 1024
        ),
    )(*arrays)


def lane_maps(quarters, parts, inner_k, inner_j):
    grid = np.indices((quarters, 2, parts, inner_k, inner_j)).reshape(5, -1)
    return grid[0] * inner_j + grid[4], grid[2] * inner_k + grid[3], grid[1]


def spectral_tables(count_x, count_y, count_z, cells_x, cells_y, cells_z, group):
    keep = MODES
    signed = np.where(np.arange(keep) < keep // 2, np.arange(keep), np.arange(keep) - keep)
    mode_j, mode_k, imaginary = lane_maps(count_x, count_y, keep // count_y, keep // count_x)
    turn = 2.0 * np.pi / GRID
    rows_y = LANES // cells_z
    place_z, row_y, cell_z = np.indices((count_z, rows_y, cells_z)).reshape(3, -1)
    phase = turn * (
        (signed[mode_j] * row_y[:, None] + mode_k * (place_z * cells_z + cell_z)[:, None]) % GRID
    )
    forward = np.where(imaginary, -np.sin(phase), np.cos(phase))
    weight = np.where(mode_k == 0, 1.0, 2.0)
    inverse = (np.where(imaginary, -np.sin(phase), np.cos(phase)) * weight).T
    sign = np.where(imaginary, -1.0, 1.0)
    strip = turn * ((signed[mode_j] * (rows_y * np.arange(GRID // rows_y))[:, None]) % GRID)
    strips = np.stack([np.cos(strip), np.sin(strip) * sign])
    cell = np.arange(count_x * cells_x).reshape(count_x, 1, cells_x)
    angle = turn * ((signed[:, None] * cell) % GRID)
    eye = np.eye(group)

    def expand(values):
        wide = np.einsum("pab,cd->pacbd", values, eye)
        return wide.reshape(count_x, values.shape[1] * group, values.shape[2] * group)

    ahead = np.concatenate([expand(np.cos(angle)), expand(np.sin(angle))], axis=2)
    back = np.swapaxes(angle, 1, 2)
    back = np.concatenate([expand(np.cos(back)), expand(np.sin(back))], axis=2)
    partner = (keep - mode_j) % keep
    same = (
        (mode_j[:, None] == partner[None, :])
        & (mode_k[:, None] == 0)
        & (mode_k[None, :] == 0)
        & (imaginary[:, None] == imaginary[None, :])
        & (mode_j[:, None] != keep // 2)
    )
    flip = same * sign[None, :]
    power = np.where(mode_k == 0, 0.5, 2.0)
    lanes = np.stack([sign, power])
    narrow = lambda array: jnp.asarray(array.astype(np.float32), jnp.bfloat16)
    single = lambda array: jnp.asarray(array.astype(np.float32))
    return (
        narrow(forward),
        narrow(inverse),
        single(strips),
        narrow(ahead),
        narrow(back),
        narrow(flip),
        single(lanes),
    )


def swap_halves(values):
    return jnp.concatenate(
        [
            pltpu.roll(values[:, at : at + LANES], LANES // 2, 1)
            for at in range(0, values.shape[1], LANES)
        ],
        axis=1,
    )


def split(values):
    upper = values.astype(jnp.bfloat16)
    return upper, (values - upper.astype(jnp.float32)).astype(jnp.bfloat16)


def spectral_kernel(
    count_x,
    count_y,
    count_z,
    lat_ref,
    weight_from,
    forward_ref,
    inverse_ref,
    strips_ref,
    ahead_ref,
    back_ref,
    flip_ref,
    lanes_ref,
    out_ref,
    came,
    plane,
    sums,
    sums_in,
    own,
    own_in,
    turned,
    mixed,
    mixed_in,
    joined,
    all_modes,
    pieces,
    weight_ref,
    fetched,
    send_a, recv_a, send_b, recv_b, send_c, recv_c, send_d, recv_d, send_e, recv_e, send_f, recv_f,
):
    place_x, place_y, place_z = lax.axis_index("gx"), lax.axis_index("gy"), lax.axis_index("gz")
    members = count_y * count_z
    me = place_y * count_z + place_z
    group = SUB
    strip_rows = plane.shape[0]
    half_modes = MODES // count_z
    inner = (MODES // count_x) * (MODES // count_y)
    mesh_id = pl.DeviceIdType.MESH

    def member(t):
        other = lax.rem(me + t, members)
        return other, {"gy": other // count_z, "gz": lax.rem(other, count_z)}

    def column(t):
        other = lax.rem(place_x + t, count_x)
        return other, {"gx": other}

    fetch = pltpu.make_async_copy(weight_from, weight_ref, fetched)
    fetch.start()
    barrier = pltpu.get_barrier_semaphore()
    for t in range(1, members):
        pl.semaphore_signal(barrier, inc=1, device_id=member(t)[1], device_id_type=mesh_id)
    for t in range(1, count_x):
        pl.semaphore_signal(barrier, inc=1, device_id=column(t)[1], device_id_type=mesh_id)
    pl.semaphore_wait(barrier, members - 1 + count_x - 1)

    def exchange_with(peer, total, source, target, send, recv):
        copies = []
        for t in range(1, total):
            other, device = peer(t)
            copy = pltpu.make_async_remote_copy(
                src_ref=source(other),
                dst_ref=target,
                send_sem=send.at[t],
                recv_sem=recv.at[t],
                device_id=device,
                device_id_type=mesh_id,
            )
            copy.start()
            copies.append(copy)
        return copies

    def apart(d, e):
        other = {
            "gy": lax.rem(place_y + count_y - d, count_y),
            "gz": lax.rem(place_z + e, count_z),
        }
        return other["gy"] * count_z + other["gz"], other

    def send_to(d, e, source, target, send, recv):
        other, device = apart(d, e)
        copy = pltpu.make_async_remote_copy(
            src_ref=source.at[other],
            dst_ref=target.at[me],
            send_sem=send.at[d * count_z + e],
            recv_sem=recv.at[d * count_z + e],
            device_id=device,
            device_id_type=mesh_id,
        )
        copy.start()
        return copy

    steps = [(d, e) for d in range(count_y) for e in range(count_z)]
    arrivals = {s: send_to(*s, lat_ref, came, send_a, recv_a) for s in steps if s != (0, 0)}
    came[me] = lat_ref[me]
    sign = lanes_ref[0:1, :]
    plane[...] = jnp.zeros_like(plane)
    chunks = came.shape[1] // strip_rows

    def ahead_step(source, chunk, carry):
        strip = source * chunks + chunk
        at = pl.multiple_of(chunk * strip_rows, strip_rows)
        block = jnp.concatenate(
            [came[source * count_z + z, pl.ds(at, strip_rows), :] for z in range(count_z)], axis=1
        )
        part = jnp.dot(block, forward_ref[...], preferred_element_type=jnp.float32)
        cosine = strips_ref[0, pl.ds(strip, 1), :]
        sine = strips_ref[1, pl.ds(strip, 1), :]
        plane[...] += part * cosine + swap_halves(part) * sine
        return carry

    for d in range(count_y):
        for e in range(count_z):
            if (d, e) in arrivals:
                arrivals[d, e].wait()
        source = lax.rem(place_y + d, count_y)
        lax.fori_loop(0, chunks, functools.partial(ahead_step, source), 0)
    lane_ids = lax.broadcasted_iota(jnp.int32, (strip_rows, LANES), 1)
    for q in range(count_x):
        part = plane[:, LANES * q : LANES * (q + 1)]
        if q == 0:
            rest = part - part.astype(jnp.bfloat16).astype(jnp.float32)
            part = jnp.where(lane_ids == LANES // 2, pltpu.roll(rest, LANES // 2, 1), part)
        sums[q] = part.astype(jnp.bfloat16)
    copies = exchange_with(column, count_x, lambda p: sums.at[p], sums_in.at[place_x], send_b, recv_b)
    sums_in[place_x] = sums[place_x]
    for copy in copies:
        copy.wait()
    constant_lane = jnp.logical_and(lane_ids == 0, place_x == 0)
    rest_lane = jnp.logical_and(lane_ids == LANES // 2, place_x == 0)
    spectrum = None
    for q in range(count_x):
        part = sums_in[q].astype(jnp.float32)
        part = part + jnp.where(constant_lane, pltpu.roll(part, LANES // 2, 1), 0.0)
        part = jnp.where(rest_lane, 0.0, part)
        for piece in split(part):
            turn = pltpu.roll(piece.astype(jnp.float32), LANES // 2, 1) * sign[:, :LANES]
            term = jnp.dot(
                ahead_ref[q],
                jnp.concatenate([piece, turn.astype(jnp.bfloat16)], axis=0),
                preferred_element_type=jnp.float32,
            )
            spectrum = term if spectrum is None else spectrum + term
    half_rows = half_modes * group
    for z in range(count_z):
        own[z] = spectrum[half_rows * z : half_rows * (z + 1)].astype(jnp.bfloat16)

    copies = exchange_with(
        member, members, lambda p: own.at[lax.rem(p, count_z)], own_in.at[me], send_c, recv_c
    )
    own_in[me] = own[place_z]
    mixed_rows = lax.broadcasted_iota(jnp.int32, (2 * inner, LANES), 0) % inner
    mixed_lanes = lax.broadcasted_iota(jnp.int32, (2 * inner, LANES), 1) // (LANES // 2)
    modes_j = MODES // count_x
    modes_k = MODES // count_y
    row_mode = (mixed_rows % modes_j) * modes_k + mixed_rows // modes_j
    first_place = (place_x + place_y + place_z) == 0
    mode_zero = lax.broadcasted_iota(jnp.int32, (inner, LANES // 2), 0) == 0
    turned[...] = jnp.zeros_like(turned)
    for copy in copies:
        copy.wait()
    fetch.wait()
    arrived = [own_in[p].astype(jnp.float32) for p in range(members)]
    for i in range(half_modes):
        column_values = jnp.concatenate([a[group * i : group * (i + 1)] for a in arrived], axis=0)
        column_values = jnp.concatenate([column_values, column_values], axis=0)
        mixed[i] = column_values.T
        at = pl.multiple_of(place_y * inner, inner)
        both = jnp.concatenate(
            [mixed[i, pl.ds(at, inner), :], mixed[i, pl.ds(LANES // 2 + at, inner), :]], axis=0
        )
        wide = jnp.concatenate(
            [
                jnp.where(row_mode == 2 * t + mixed_lanes, both, 0.0).astype(jnp.bfloat16)
                for t in range(inner // 2)
            ],
            axis=1,
        )
        by_real = jnp.dot(wide, weight_ref[0, i], preferred_element_type=jnp.float32)
        by_imag = jnp.dot(wide, weight_ref[1, i], preferred_element_type=jnp.float32)
        real = by_real[:inner] - by_imag[inner:]
        imag = by_imag[:inner] + by_real[inner:]
        if i == 0:
            drop = jnp.logical_and(mode_zero, first_place)
            real = jnp.where(drop, 0.0, real)
            imag = jnp.where(drop, 0.0, imag)
        turned[i, pl.ds(at, inner), 0 : LANES // 2] = real
        turned[i, pl.ds(LANES // 2 + at, inner), 0 : LANES // 2] = imag
    flat = [turned[i].T for i in range(half_modes)]
    for p in range(members):
        joined[p] = jnp.concatenate(
            [f[group * p : group * (p + 1)] for f in flat], axis=0
        ).astype(jnp.bfloat16)

    copies = exchange_with(member, members, lambda p: joined.at[p], mixed_in.at[me], send_d, recv_d)
    mixed_in[me] = joined[me]
    for copy in copies:
        copy.wait()
    parts = []
    for z in range(count_z):
        value = mixed_in[z].astype(jnp.float32)
        for y in range(1, count_y):
            value = value + mixed_in[y * count_z + z].astype(jnp.float32)
        parts.append(value)
    all_modes[place_x] = jnp.concatenate(parts, axis=0).astype(jnp.bfloat16)
    copies = exchange_with(
        column, count_x, lambda p: all_modes.at[place_x], all_modes.at[place_x], send_e, recv_e
    )
    for copy in copies:
        copy.wait()
    modes = jnp.concatenate([all_modes[q] for q in range(count_x)], axis=1)
    scaled = modes.astype(jnp.float32) * (1.0 / GRID**3)
    partner = jnp.dot(modes, flip_ref[...], preferred_element_type=jnp.float32) * (1.0 / GRID**3)
    energy = None
    for i in range(MODES):
        value = scaled[group * i : group * (i + 1)]
        term = value * value * lanes_ref[1:2, :]
        if i != MODES // 2:
            other = (MODES - i) % MODES
            term = term + 0.5 * value * partner[group * other : group * (other + 1)]
        energy = term if energy is None else energy + term
    variance = jnp.sum(energy, axis=1, keepdims=True)
    gain = 1.0 / jnp.sqrt(variance + NORM_FLOOR)
    rotated = (swap_halves(scaled * float(GRID**3)) * -sign).astype(jnp.bfloat16)
    back = jnp.dot(
        back_ref[place_x], jnp.concatenate([modes, rotated], axis=0), preferred_element_type=jnp.float32
    )
    back = back.reshape(-1, group, back.shape[1]) * (gain * (1.0 / GRID**3))[None]
    plane[...] = back.reshape(plane.shape)

    def back_step(source, chunk, carry):
        strip = source * chunks + chunk
        at = pl.multiple_of(chunk * strip_rows, strip_rows)
        cosine = strips_ref[0, pl.ds(strip, 1), :]
        sine = strips_ref[1, pl.ds(strip, 1), :]
        value = plane[...]
        value = (value * cosine - swap_halves(value) * sine).astype(jnp.bfloat16)
        result = jnp.dot(value, inverse_ref[...], preferred_element_type=jnp.float32)
        for z in range(count_z):
            pieces[source * count_z + z, pl.ds(at, strip_rows), :] = result[
                :, LANES * z : LANES * (z + 1)
            ].astype(jnp.bfloat16)
        return carry

    copies = []
    for d in [*range(1, count_y), 0]:
        source = lax.rem(place_y + count_y - d, count_y)
        lax.fori_loop(0, chunks, functools.partial(back_step, source), 0)
        copies += [
            send_to(d, e, pieces, out_ref, send_f, recv_f) for e in range(count_z) if (d, e) != (0, 0)
        ]
    out_ref[me] = pieces[me]
    for copy in copies:
        copy.wait()


def spectral_branch(lat, spectral):
    count_x, count_y, count_z = (lax.axis_size(a) for a in ("gx", "gy", "gz"))
    members, piece_rows, _ = lat.shape
    cells_x, cells_y, cells_z = GRID // count_x, GRID // count_y, GRID // count_z
    strip_rows = cells_x * SUB
    half_modes = MODES // count_z
    channels = spectral.shape[-1]
    inner = (MODES // count_x) * (MODES // count_y)
    lanes = 2 * MODES * MODES
    tables = spectral_tables(count_x, count_y, count_z, cells_x, cells_y, cells_z, SUB)
    weight = spectral.reshape(2, half_modes, inner * channels, channels)
    vmem = lambda: pl.BlockSpec(memory_space=pltpu.VMEM)
    half = half_modes * SUB
    dma = pltpu.SemaphoreType.DMA
    return pl.pallas_call(
        functools.partial(spectral_kernel, count_x, count_y, count_z),
        out_shape=jax.ShapeDtypeStruct(lat.shape, jnp.bfloat16),
        in_specs=[vmem(), pl.BlockSpec(memory_space=pltpu.HBM)] + [vmem() for _ in range(7)],
        out_specs=vmem(),
        scratch_shapes=[
            pltpu.VMEM(lat.shape, jnp.bfloat16),
            pltpu.VMEM((strip_rows, lanes), jnp.float32),
            pltpu.VMEM((count_x, strip_rows, LANES), jnp.bfloat16),
            pltpu.VMEM((count_x, strip_rows, LANES), jnp.bfloat16),
            pltpu.VMEM((count_z, half, LANES), jnp.bfloat16),
            pltpu.VMEM((members, half, LANES), jnp.bfloat16),
            pltpu.VMEM((half_modes, LANES, LANES), jnp.float32),
            pltpu.VMEM((half_modes, LANES, LANES), jnp.float32),
            pltpu.VMEM((members, half, LANES), jnp.bfloat16),
            pltpu.VMEM((members, half, LANES), jnp.bfloat16),
            pltpu.VMEM((count_x, MODES * SUB, LANES), jnp.bfloat16),
            pltpu.VMEM(lat.shape, jnp.bfloat16),
            pltpu.VMEM(weight.shape, weight.dtype),
            dma,
        ]
        + [dma((members,))] * 2
        + [dma((count_x,))] * 2
        + [dma((members,))] * 2
        + [dma((members,))] * 2
        + [dma((count_x,))] * 2
        + [dma((members,))] * 2,
        compiler_params=pltpu.CompilerParams(
            collective_id=0, has_side_effects=True, vmem_limit_bytes=48 * 1024 * 1024
        ),
    )(lat, weight, *tables)


def final_kernel(branch_ref, lat_ref, skip_ref, out_ref):
    members = branch_ref.shape[0]
    count = out_ref.shape[0]
    rows = count * SUB
    part = pl.ds(pl.multiple_of(pl.program_id(0) * rows, rows), rows)
    branch = [branch_ref[p, part, :].astype(jnp.float32) for p in range(members)]
    latent = [lat_ref[p, part, :].astype(jnp.float32) for p in range(members)]
    pick = lambda parts, x: jnp.concatenate([a[SUB * x : SUB * (x + 1)] for a in parts], axis=0)
    wide = jnp.concatenate([pick(latent, x) for x in range(count)], axis=1).astype(jnp.bfloat16)
    turned = skip_ref[...].astype(jnp.float32).T.astype(jnp.bfloat16)
    skip = jnp.dot(turned, wide, preferred_element_type=jnp.float32)
    for x in range(count):
        v = pick(branch, x) + skip[:, LANES * x : LANES * (x + 1)]
        inner = v * (0.7978845608028654 + 0.035677408136300125 * (v * v))
        half = 0.5 * v
        out_ref[x, 0] = (half + half * jnp.tanh(inner)).T


def finish(branch, lat, skip_weight, cells_x):
    members, piece_rows, _ = lat.shape
    channels = skip_weight.shape[0]
    rows = cells_x * SUB
    whole = pl.BlockSpec(memory_space=pltpu.VMEM)
    return pl.pallas_call(
        final_kernel,
        grid=(piece_rows // rows,),
        out_shape=jax.ShapeDtypeStruct((cells_x, piece_rows // rows, LANES, channels), jnp.float32),
        in_specs=[whole, whole, whole],
        out_specs=pl.BlockSpec((cells_x, 1, LANES, channels), lambda i: (0, i, 0, 0)),
        compiler_params=pltpu.CompilerParams(vmem_limit_bytes=24 * 1024 * 1024),
    )(branch, lat, skip_weight)


def summed_over_axes(values, axes):
    for axis in axes:
        count = lax.axis_size(axis)
        copies = jnp.broadcast_to(values[None], (count,) + values.shape)
        values = jnp.sum(lax.all_to_all(copies, axis, 0, 0, tiled=True), axis=0)
    return values


def exchange(values, axis, split_axis, concat_axis):
    return lax.all_to_all(
        values.astype(jnp.bfloat16), axis, split_axis=split_axis, concat_axis=concat_axis, tiled=True
    ).astype(jnp.float32)


def body(point_data, neighbours, counts, kernel_in, kernel_mid, kernel_out, spectral, skip_weight):
    count_y = lax.axis_size("gy")
    count_z = lax.axis_size("gz")
    place_x = lax.axis_index("gx")
    place_y = lax.axis_index("gy")
    place_z = lax.axis_index("gz")
    geometry_count, cells_x, cells_y, cells_z = neighbours.shape[0:4]
    per_device = point_data.shape[2]
    channels = skip_weight.shape[0]
    rows_y = LANES // cells_z
    shape = (cells_x, cells_y, cells_z)
    node_order = lambda values: jnp.swapaxes(
        values.reshape(cells_x, cells_y // rows_y, LANES), 0, 1
    ).reshape(-1, LANES)
    grouped = (
        count_y * count_z * SUB == channels
        and cells_x * SUB == LANES
        and count_z * MODES // 2 == MODES
        and 2 * (MODES // lax.axis_size("gx")) * MODES == LANES
    )
    latent = []
    for geometry in range(geometry_count):
        latent.append(
            encode(
                node_order(counts[geometry]),
                *prepare(
                    point_data[geometry], neighbours[geometry], kernel_in, kernel_mid, kernel_out
                ),
                shape,
                grouped,
            )
        )
    if grouped:
        results = [
            finish(spectral_branch(lat, spectral), lat, skip_weight, cells_x) for lat in latent
        ]
        return jnp.stack(results).reshape(geometry_count, cells_x, cells_y, cells_z, channels)
    latent = jnp.swapaxes(jnp.stack(latent), 2, 3).astype(jnp.bfloat16)
    latent = latent.reshape(geometry_count, cells_y // rows_y, cells_x, LANES, channels)
    latent = jnp.swapaxes(latent, 1, 2)
    latent = latent.reshape(geometry_count, cells_x, cells_y, cells_z, channels)
    cos_centred, sin_centred = tables(GRID, MODES, True)
    cos_third, sin_third = tables(GRID, MODES, False)
    back_cos, back_sin = third_weights(cos_third, sin_third, GRID)
    depth_full = lax.all_to_all(latent, "gz", split_axis=4, concat_axis=3, tiled=True)
    real_part, imag_part = forward_real(
        depth_full.astype(jnp.float32), cos_third, sin_third, "gxyzc,kz->gxykc"
    )
    real_part, imag_part = (
        lax.all_to_all(real_part, "gy", split_axis=3, concat_axis=2, tiled=True),
        lax.all_to_all(imag_part, "gy", split_axis=3, concat_axis=2, tiled=True),
    )
    real_part, imag_part = forward_complex(
        real_part, imag_part, cos_centred, sin_centred, "gxykc,jy->gxjkc"
    )
    real_part, imag_part = (
        lax.all_to_all(real_part, "gx", split_axis=2, concat_axis=1, tiled=True),
        lax.all_to_all(imag_part, "gx", split_axis=2, concat_axis=1, tiled=True),
    )
    real_part, imag_part = forward_complex(
        real_part, imag_part, cos_centred, sin_centred, "gxjkc,ix->gijkc"
    )
    spec_real, spec_imag = (
        exchange(real_part, "gz", split_axis=1, concat_axis=4),
        exchange(imag_part, "gz", split_axis=1, concat_axis=4),
    )
    spec_real = spec_real.astype(jnp.bfloat16)
    spec_imag = spec_imag.astype(jnp.bfloat16)
    mixed_real = jnp.einsum(
        "gijkc,ijkco->gijko", spec_real, spectral[0], preferred_element_type=jnp.float32
    ) - jnp.einsum("gijkc,ijkco->gijko", spec_imag, spectral[1], preferred_element_type=jnp.float32)
    mixed_imag = jnp.einsum(
        "gijkc,ijkco->gijko", spec_real, spectral[1], preferred_element_type=jnp.float32
    ) + jnp.einsum("gijkc,ijkco->gijko", spec_imag, spectral[0], preferred_element_type=jnp.float32)
    first_place = (place_x + place_y + place_z) == 0
    modes = mixed_real.shape[1:4]
    order = sum(lax.broadcasted_iota(jnp.int32, modes, d) for d in range(3))
    zero_mode = ((order == 0) & first_place)[None, ..., None]
    mixed_real = jnp.where(zero_mode, 0.0, mixed_real)
    mixed_imag = jnp.where(zero_mode, 0.0, mixed_imag)
    mixed_real = mixed_real.astype(jnp.bfloat16)
    mixed_imag = mixed_imag.astype(jnp.bfloat16)
    real_part, imag_part = (
        exchange(mixed_real, "gz", split_axis=4, concat_axis=1),
        exchange(mixed_imag, "gz", split_axis=4, concat_axis=1),
    )
    real_part, imag_part = inverse_complex(
        real_part.astype(jnp.float32),
        imag_part.astype(jnp.float32),
        cos_centred,
        sin_centred,
        "gijkc,ix->gxjkc",
    )
    real_part, imag_part = (
        exchange(real_part, "gx", split_axis=1, concat_axis=2),
        exchange(imag_part, "gx", split_axis=1, concat_axis=2),
    )
    real_part, imag_part = inverse_complex(
        real_part, imag_part, cos_centred, sin_centred, "gxjkc,jy->gxykc"
    )
    real_part, imag_part = (
        exchange(real_part, "gy", split_axis=2, concat_axis=3),
        exchange(imag_part, "gy", split_axis=2, concat_axis=3),
    )
    depth_part = inverse_real(real_part, imag_part, back_cos, back_sin, "gxykc,kz->gxyzc")
    branch = exchange(depth_part, "gz", split_axis=3, concat_axis=4)
    skip = jnp.einsum("gxyzc,co->gxyzo", latent, skip_weight, preferred_element_type=jnp.float32)
    cells_total = float(GRID**3)
    variance = (
        summed_over_axes(jnp.sum(branch * branch, axis=(1, 2, 3)), ("gz", "gy", "gx")) / cells_total
    )
    normed = branch / jnp.sqrt(variance + NORM_FLOOR)[:, None, None, None, :]
    return jax.nn.gelu(normed + skip, approximate=True)


def solution(mesh):
    in_specs = (
        P(None, None, ("gx", "gy", "gz")),
        P(None, "gx", "gy", "gz", None),
        P(None, "gx", "gy", "gz"),
        P(),
        P(),
        P(),
        P(None, "gz", "gx", "gy", None, None),
        P(),
    )
    out_specs = P(None, "gx", "gy", "gz", None)
    return jax.shard_map(body, mesh=mesh, in_specs=in_specs, out_specs=out_specs, check_vma=False)
```
